256 devices in a mesh: gx: 8 (over z), gy: 4 (over x), gz: 8 (over y, core).
Axes of the slice: x: 4, y: 4, z: 8, core: 2. Of those that a mesh axis runs over, the one named last changes fastest.
Arguments:
- east_wind: float32 [96, 1024, 512], P('gz', 'gx', 'gy'), may hold values from -6 to 6
- north_wind: float32 [96, 1024, 512], P('gz', 'gx', 'gy'), may hold values from -6 to 6
- vertical_wind: float32 [96, 1024, 512], P('gz', 'gx', 'gy'), may hold values from -6 to 6
- geopotential: float32 [96, 1024, 512], P('gz', 'gx', 'gy'), may hold values from -6 to 6
- pressure: float32 [96, 1024, 512], P('gz', 'gx', 'gy'), may hold values from -6 to 6
- column_mass: float32 [1024, 512], P('gx', 'gy'), may hold values from 0.5 to 2
Outputs:
- east_after: float32 [96, 1024, 512], P('gz', 'gx', 'gy')
- north_after: float32 [96, 1024, 512], P('gz', 'gx', 'gy')
- vertical_after: float32 [96, 1024, 512], P('gz', 'gx', 'gy')
- geo_after: float32 [96, 1024, 512], P('gz', 'gx', 'gy')
- pressure_after: float32 [96, 1024, 512], P('gz', 'gx', 'gy')
The draws below stay inside these ranges and needn't reach their ends.
All inputs are finite; a program needn't handle non-finite values.
Results may differ from the reference program's by a relative error of at most 0.0003.
Values sent between devices are 32-bit elements; how exact they have to be, the bound alone decides.
No kernel may reach another device: no remote copies, remote signals or barrier semaphores. Data moves between devices by JAX's collectives and lax.ppermute only.
A program may use at most 64 MiB of HBM per device.

```python
import math
import jax
import jax.numpy as jnp
from jax import lax

NZ = 96
ITERS = 3
NX = 1024
NY = 512


def draw_vertical_wind(key, part):
    key_noise = jax.random.fold_in(key, 11)
    noise = jax.random.truncated_normal(key_noise, -6.0, 6.0, (NZ, NX, NY), jnp.float32)
    return noise


def steps_of(own_key, dims, shards, low, top_value):
    gain, own = 1.0, jax.random.fold_in(own_key, 6)
    for dim, blocks in shards:
        draws = jnp.exp(jax.random.uniform(jax.random.fold_in(own, dim), (blocks,), jnp.float32, low / len(shards), top_value / len(shards)))
        gain = gain * jnp.repeat(draws, dims[dim] // blocks).reshape([-1 if axis == dim else 1 for axis in range(len(dims))])
    return gain


def bell_draw(rng, shape, spread, reach, pieces=(), held_as=jnp.bfloat16):
    gain = steps_of(rng, shape, pieces, -0.22, 0.18) if pieces else 1.0
    drawn = jax.random.normal(rng, shape, jnp.float32) * spread * gain
    return jnp.minimum(jnp.maximum(drawn, -reach), reach).astype(held_as)


def setup_inputs(seed: int = 0) -> dict:
    seeds = jax.random.split(jax.random.key(seed), 7)
    return {
        "east_wind": bell_draw(seeds[0], (NZ, NX, NY), 1.0, 6.0, ((0, 8), (1, 8), (2, 4)), jnp.float32),
        "north_wind": bell_draw(seeds[1], (NZ, NX, NY), 1.0, 6.0, ((0, 8), (1, 8), (2, 4)), jnp.float32),
        "vertical_wind": draw_vertical_wind(jax.random.fold_in(seeds[6], 71), 0),
        "geopotential": bell_draw(seeds[3], (NZ, NX, NY), 1.0, 6.0, ((0, 8), (1, 8), (2, 4)), jnp.float32),
        "pressure": bell_draw(seeds[4], (NZ, NX, NY), 1.0, 6.0, ((0, 8), (1, 8), (2, 4)), jnp.float32),
        "column_mass": jnp.clip(jnp.exp(math.log(2.0) - 1.3862944 * jax.random.uniform(seeds[5], (NX, NY), jnp.float32) ** steps_of(seeds[5], (NX, NY), ((0, 8), (1, 4)), -0.2, 0.2)), 0.5, 2.0),
    }


horiz_push = 0.25
mass_flux = 0.2
level_push = 1.0
buoy_coupling = 0.5
geo_rate = 0.5
level_flux = 0.5
stiffness = 30.0


def centered(source, dim_index):
    return jnp.roll(source, -1, dim_index) - jnp.roll(source, 1, dim_index)


def level_diff(source):
    zeros_level = jnp.zeros_like(source[:1])
    shifted_up = jnp.concatenate([source[1:], zeros_level], 0)
    shifted_down = jnp.concatenate([zeros_level, source[:-1]], 0)
    return shifted_up - shifted_down


def column_solve(forcing, stiff_ratio):
    diagonal = 1.0 + 2.0 * stiff_ratio

    def forward(carried, forcing_row):
        coef_prev, rhs_prev = carried
        pivot_row = diagonal + stiff_ratio * coef_prev
        coef_next = -stiff_ratio / pivot_row
        rhs_next = (forcing_row + stiff_ratio * rhs_prev) / pivot_row
        return (coef_next, rhs_next), (coef_next, rhs_next)

    zeros_plane = jnp.zeros_like(stiff_ratio)
    _, (coefs, rhs_rows) = lax.scan(forward, (zeros_plane, zeros_plane), forcing)

    def backward(next_value, level_item):
        coef_row, rhs_row = level_item
        solved = rhs_row - coef_row * next_value
        return solved, solved

    _, solved = lax.scan(backward, zeros_plane, (coefs, rhs_rows), reverse=True)
    return solved


def reference(east_wind, north_wind, vertical_wind, geopotential, pressure, column_mass):
    stiff_ratio = stiffness * column_mass
    for substep in range(ITERS):
        east_wind = east_wind - horiz_push * centered(pressure, 1)
        north_wind = north_wind - horiz_push * centered(pressure, 2)
        divergence = centered(east_wind, 1) + centered(north_wind, 2)
        pressure_star = pressure - mass_flux * column_mass * divergence
        forcing = vertical_wind - level_push * level_diff(pressure_star) + buoy_coupling * geopotential
        vertical_wind = column_solve(forcing, stiff_ratio)
        geopotential = geopotential + geo_rate * vertical_wind
        pressure = pressure_star - level_flux * column_mass * level_diff(vertical_wind)
    return east_wind, north_wind, vertical_wind, geopotential, pressure
```

```python
import functools

import jax
import jax.numpy as jnp
from jax import lax
from jax.experimental import pallas as pl
from jax.experimental.pallas import tpu as pltpu
from jax.sharding import PartitionSpec as P

ITERS = 3

horiz_push = 0.25
mass_flux = 0.2
buoy_coupling = 0.5
geo_rate = 0.5
level_flux = 0.5
stiffness = 30.0


F32 = jnp.float32
NZ = 96
LV = 24
HALF = 12
RX = 64
LN = 128
TILES = RX // 8
VMEM = pl.BlockSpec(memory_space=pltpu.VMEM)
ANY = pl.BlockSpec(memory_space=pl.ANY)


def shape(*dims):
    return jax.ShapeDtypeStruct(dims, F32)


def call(body, outs, args, in_specs=None, scratch=(), cost=2_000_000, out_specs=None):
    return pl.pallas_call(
        body,
        out_shape=outs,
        in_specs=in_specs or [VMEM] * len(args),
        out_specs=out_specs or [VMEM] * len(outs),
        scratch_shapes=list(scratch),
        cost_estimate=pl.CostEstimate(flops=cost, bytes_accessed=1_000_000, transcendentals=0),
        compiler_params=pltpu.CompilerParams(vmem_limit_bytes=24 * 1024 * 1024),
    )(*args)


def core_of():
    return lax.rem(lax.axis_index("gz"), 2)


def chip_of():
    return lax.div(lax.axis_index("gz"), 2)


def lanes(rows=8):
    return lax.broadcasted_iota(jnp.int32, (rows, LN), 1)


def roll_lanes(value, amount):
    return pltpu.roll(value, amount % LN, 1)


def split_kernel(count, *refs):
    ins, (own, send, sem) = refs[:count], refs[count:]
    core = core_of()
    copies = []
    for f in range(count):
        for which, out in ((1 - core, send), (core, own)):
            rows = pl.ds(pl.multiple_of(which * RX, RX), RX)
            copy = pltpu.make_async_copy(ins[f].at[:, rows, :], out.at[f], sem.at[len(copies)])
            copy.start()
            copies.append(copy)
    for copy in copies:
        copy.wait()


def split(fields):
    count = len(fields)
    return call(
        functools.partial(split_kernel, count),
        [shape(count, HALF, RX, LN)] * 2,
        fields,
        in_specs=[ANY] * count,
        scratch=[pltpu.SemaphoreType.DMA((2 * count,))],
        cost=100_000,
    )


def merge_kernel(count, own, got, *refs):
    outs, sem = refs[:count], refs[count]
    core = core_of()
    copies = []
    for f in range(count):
        for which, src in ((core, own), (1 - core, got)):
            rows = pl.ds(pl.multiple_of(which * RX, RX), RX)
            copy = pltpu.make_async_copy(src.at[f], outs[f].at[:, rows, :], sem.at[len(copies)])
            copy.start()
            copies.append(copy)
    for copy in copies:
        copy.wait()


def merge(own, got):
    count = own.shape[0]
    return call(
        functools.partial(merge_kernel, count),
        [shape(HALF, 2 * RX, LN)] * count,
        [own, got],
        out_specs=[ANY] * count,
        scratch=[pltpu.SemaphoreType.DMA((2 * count,))],
        cost=100_000,
    )


def pack_columns(get_level, out, base):
    lane = lanes()

    def group(g, carry):
        acc = jnp.zeros((8, LN), F32)
        for j in range(4):
            value = get_level(4 * g + j)
            for t in range(TILES):
                slot = 8 * j + t
                moved = roll_lanes(value[8 * t : 8 * t + 8], 4 * slot - 126)
                acc = jnp.where(lane // 4 == slot, moved, acc)
        out[pl.ds(pl.multiple_of(base + 8 * g, 8), 8), :] = acc
        return carry

    lax.fori_loop(0, LV // 4, group, 0)


def pack_rows(get_level, mid, outer, base):
    core = core_of()

    def group(g, carry):
        first, last = [], []
        for j in range(4):
            value = get_level(4 * g + j)
            first.append(value[0:2])
            last.append(value[RX - 2 : RX])
        first, last = jnp.concatenate(first, 0), jnp.concatenate(last, 0)
        rows = pl.ds(pl.multiple_of(base + 8 * g, 8), 8)
        mid[rows, :] = jnp.where(core == 0, last, first)
        outer[rows, :] = jnp.where(core == 0, first, last)
        return carry

    lax.fori_loop(0, LV // 4, group, 0)


def join_kernel(own, got, press, east, north, mid, outer, cols):
    core = core_of()
    here, there = core * HALF, (1 - core) * HALF

    def level(k, carry):
        for f, out in enumerate((press, east, north)):
            out[here + k] = own[f, k]
            out[there + k] = got[f, k]
        return carry

    lax.fori_loop(0, HALF, level, 0)
    pack_rows(lambda k: press[k], mid, outer, 0)
    pack_rows(lambda k: east[k], mid, outer, 2 * LV)
    pack_columns(lambda k: press[k], cols, 0)
    pack_columns(lambda k: north[k], cols, 2 * LV)


def join_wind_kernel(own, got, wind, geo):
    core = core_of()
    here, there = core * HALF, (1 - core) * HALF

    def level(k, carry):
        for f, out in enumerate((wind, geo)):
            out[here + k] = own[f, k]
            out[there + k] = got[f, k]
        return carry

    lax.fori_loop(0, HALF, level, 0)


def spread_columns(packed, j):
    return jnp.concatenate(
        [roll_lanes(packed, 126 - 4 * (8 * j + t)) for t in range(TILES)], 0
    )


def stage_one_kernel(first, *refs):
    (press, east, north, wind, geo, mass, rate, scale, up, down, mid_in, outer_in, left, right, own_cols) = refs[:15]
    refs = refs[15:]
    if not first:
        (east_edge, north_edge), refs = refs[:2], refs[2:]
    (east_out, north_out, east_edge_out, north_edge_out, star, forced, to_next, to_far, to_prev) = refs[:9]
    pbuf, ebuf = refs[9:]
    core, chip = core_of(), chip_of()
    lane = lanes()
    wide = lanes(RX)
    quarter = lane % 4

    def group(g, carry):
        rows = pl.ds(pl.multiple_of(8 * g, 8), 8)
        more = pl.ds(pl.multiple_of(2 * LV + 8 * g, 8), 8)
        p_low = jnp.where(core == 0, outer_in[rows, :], mid_in[rows, :])
        p_high = jnp.where(core == 0, mid_in[rows, :], outer_in[rows, :])
        if first:
            e_low = jnp.where(core == 0, outer_in[more, :], mid_in[more, :])
            e_high = jnp.where(core == 0, mid_in[more, :], outer_in[more, :])
            odd = lax.broadcasted_iota(jnp.int32, (8, LN), 0) % 2
            n_edge = jnp.where(quarter < 2, left[more, :], right[more, :])
            e_edge = jnp.where(odd == 1, e_low, e_high)
        else:
            e_edge = east_edge[rows, :]
            n_edge = north_edge[rows, :]
        p_edge = jnp.where(quarter < 2, left[rows, :], right[rows, :])
        p_own = own_cols[rows, :]
        n_edge = n_edge - horiz_push * jnp.where(
            quarter == 1,
            roll_lanes(p_own, -1) - roll_lanes(p_edge, 1),
            roll_lanes(p_edge, -1) - roll_lanes(p_own, 1),
        )
        north_edge_out[rows, :] = n_edge
        edges = []
        for j in range(4):
            k = 4 * g + j
            p = press[k]
            pbuf[j, 8 : 8 + RX, :] = p
            pbuf[j, 6:8, :] = p_low[2 * j : 2 * j + 2]
            pbuf[j, 8 + RX : 10 + RX, :] = p_high[2 * j : 2 * j + 2]
            e_new = east[k] - horiz_push * (pbuf[j, 9 : 9 + RX, :] - pbuf[j, 7 : 7 + RX, :])
            e_under = e_edge[2 * j + 1 : 2 * j + 2] - horiz_push * (p[0:1] - p_low[2 * j : 2 * j + 1])
            e_over = e_edge[2 * j : 2 * j + 1] - horiz_push * (p_high[2 * j + 1 : 2 * j + 2] - p[RX - 1 : RX])
            edges += [e_over, e_under]
            ebuf[j, 8 : 8 + RX, :] = e_new
            ebuf[j, 7:8, :] = e_under
            ebuf[j, 8 + RX : 9 + RX, :] = e_over
            east_out[k] = e_new
            spread_p = spread_columns(p_edge, j)
            spread_n = spread_columns(n_edge, j)
            n_new = north[k] - horiz_push * (
                roll_lanes(jnp.where(wide == 0, spread_p, p), -1)
                - roll_lanes(jnp.where(wide == LN - 1, spread_p, p), 1)
            )
            north_out[k] = n_new
            divergence = (ebuf[j, 9 : 9 + RX, :] - ebuf[j, 7 : 7 + RX, :]) + (
                roll_lanes(jnp.where(wide == 0, spread_n, n_new), -1)
                - roll_lanes(jnp.where(wide == LN - 1, spread_n, n_new), 1)
            )
            star[k + 1] = p - mass_flux * mass[...] * divergence
        east_edge_out[rows, :] = jnp.concatenate(edges, 0)
        return carry

    zero = jnp.zeros((RX, LN), F32)
    star[0] = zero
    star[LV + 1] = zero
    lax.fori_loop(0, LV // 4, group, 0)

    ratio = rate[0]
    shift = 0 if first else 1

    def level(k, carry):
        total, tail, power = carry
        f = scale[...] * (
            wind[k + shift] + buoy_coupling * geo[k] - (star[k + 2] - star[k])
        )
        forced[k] = f
        power = power * ratio
        return ratio * total + up[k + 1] * f, tail + power * (down[k + 1] * f), power

    inverse = rate[1]
    bottom = scale[...] * star[1]
    top = scale[...] * star[LV]
    total, tail, power = lax.fori_loop(
        0, LV, level, (-up[0] * bottom, -inverse * down[0] * bottom, inverse)
    )
    total = total + inverse * up[LV + 1] * top
    tail = tail + power * ratio * (down[LV + 1] * top)
    to_next[0] = jnp.where(chip < 3, total, tail)
    to_next[1] = top
    to_far[...] = jnp.where(chip < 2, total, tail)
    to_prev[0] = jnp.where(chip > 0, tail, total)
    to_prev[1] = bottom


def stage_one(first, *args):
    edge = shape(2 * LV, LN)
    field = shape(LV, RX, LN)
    return call(
        functools.partial(stage_one_kernel, first),
        [field, field, edge, edge, shape(LV + 2, RX, LN), field, shape(2, RX, LN), shape(RX, LN), shape(2, RX, LN)],
        args,
        scratch=[
            pltpu.VMEM((4, RX + 16, LN), F32),
            pltpu.VMEM((4, RX + 16, LN), F32),
        ],
    )


def stage_two_kernel(last, *refs):
    (star, forced, geo, mass, rate, up, down, from_prev, from_far, from_next) = refs[:10]
    refs = refs[10:]
    if last:
        (mine, theirs, sums, wind, geo_out, press) = refs
    else:
        (wind, geo_out, press, mid, outer, cols, sums) = refs
    core, chip = core_of(), chip_of()
    ratio, inverse, deep, scale = rate[0], rate[1], rate[2], rate[3]
    zero = jnp.zeros((RX, LN), F32)
    prev, far, after = from_prev[0], from_far[...], from_next[0]
    star_under = jnp.where(chip > 0, from_prev[1], zero)
    star_over = jnp.where(chip < 3, from_next[1], zero)
    far_deep = deep * far
    enter = jnp.where(
        chip == 0,
        zero,
        prev + jnp.where(chip >= 2, far_deep, zero) + jnp.where(chip == 3, deep * deep * after, zero),
    )
    above = jnp.where(
        chip == 3,
        zero,
        after + jnp.where(chip <= 1, far_deep, zero) + jnp.where(chip == 0, deep * deep * prev, zero),
    )
    enter = enter - inverse * up[1] * star_under - up[0] * (scale * star[1])
    above = above + inverse * down[LV] * star_over + down[LV + 1] * (scale * star[LV])
    lowest = forced[0] + star_under
    highest = forced[LV - 1] - star_over

    def upward(k, total):
        total = ratio * total + up[k + 1] * forced[k]
        sums[k] = total
        return total

    total = ratio * enter + up[1] * lowest
    sums[0] = total
    total = lax.fori_loop(1, LV - 1, upward, total)
    total = ratio * total + up[LV] * highest
    sums[LV - 1] = total
    wind[LV + 1] = down[LV + 1] * (ratio * total) + up[LV + 1] * above

    def settle(k, carried):
        solved = down[k + 1] * sums[k] + up[k + 1] * carried
        wind[k + 1] = solved
        geo_out[k] = geo[k] + geo_rate * solved

    def downward(step, carried):
        k = LV - 1 - step
        settle(k, carried)
        return ratio * (carried + down[k + 1] * forced[k])

    carried = ratio * above
    settle(LV - 1, carried)
    carried = ratio * (carried + down[LV] * highest)
    carried = lax.fori_loop(1, LV - 1, downward, carried)
    settle(0, carried)
    carried = ratio * (carried + down[1] * lowest)
    wind[0] = down[0] * enter + up[0] * carried

    def level(k, carry):
        press[k] = star[k + 1] - level_flux * mass[...] * (wind[k + 2] - wind[k])
        return carry

    lax.fori_loop(0, LV, level, 0)
    if last:
        here, there = core * HALF, (1 - core) * HALF

        def sort(k, carry):
            for f, (source, off) in enumerate(((wind, 1), (geo_out, 0), (press, 0))):
                mine[f, k] = source[here + k + off]
                theirs[f, k] = source[there + k + off]
            return carry

        lax.fori_loop(0, HALF, sort, 0)
    else:
        pack_rows(lambda k: press[k], mid, outer, 0)
        pack_columns(lambda k: press[k], cols, 0)


def stage_two(last, *args):
    edge = shape(2 * LV, LN)
    field = shape(LV, RX, LN)
    tall = shape(LV + 2, RX, LN)
    if last:
        outs = [shape(3, HALF, RX, LN)] * 2
        scratch = [pltpu.VMEM(s.shape, F32) for s in (field, tall, field, field)]
    else:
        outs = [tall, field, field, edge, edge, edge]
        scratch = [pltpu.VMEM(field.shape, F32)]
    return call(functools.partial(stage_two_kernel, last), outs, args, scratch=scratch)


def sort_winds_kernel(east, north, mine, theirs):
    core = core_of()
    here, there = core * HALF, (1 - core) * HALF

    def level(k, carry):
        for f, source in enumerate((east, north)):
            mine[f, k] = source[here + k]
            theirs[f, k] = source[there + k]
        return carry

    lax.fori_loop(0, HALF, level, 0)


def local(east_wind, north_wind, vertical_wind, geopotential, pressure, column_mass):
    columns, tiles, pieces = lax.axis_size("gx"), lax.axis_size("gy"), lax.axis_size("gz")
    core, chip = core_of(), chip_of()
    swap = [(i, i ^ 1) for i in range(pieces)]

    def along(distance):
        return [(i, (i + 2 * distance) % pieces) for i in range(pieces)]

    outward = [
        (a * pieces + z, (a + (1 if z % 2 else -1)) % columns * pieces + (z ^ 1))
        for a in range(columns)
        for z in range(pieces)
    ]
    east_ring = [(i, (i + 1) % tiles) for i in range(tiles)]
    west_ring = [(i, (i - 1) % tiles) for i in range(tiles)]

    own, send = split([pressure, east_wind, north_wind])
    got = lax.ppermute(send, "gz", swap)
    own_wind, send_wind = split([vertical_wind, geopotential])
    got_wind = lax.ppermute(send_wind, "gz", swap)

    mass = lax.dynamic_slice_in_dim(column_mass, core * RX, RX, 0)
    stiff_ratio = stiffness * mass
    root = jnp.sqrt(1.0 + 4.0 * stiff_ratio)
    ratio = (1.0 + 2.0 * stiff_ratio - root) / (2.0 * stiff_ratio)
    log_ratio = jnp.log(ratio)
    level = (chip * LV - 1 + lax.iota(jnp.int32, LV + 2)).astype(F32)[:, None, None]
    up = 1.0 - jnp.exp((2.0 * (level + 1.0)) * log_ratio)
    down = 1.0 - jnp.exp((2.0 * (NZ - level)) * log_ratio)
    scale = 1.0 / (root * (1.0 - jnp.exp((2.0 * (NZ + 1.0)) * log_ratio)))
    rate = jnp.stack([ratio, 1.0 / ratio, jnp.exp(float(LV) * log_ratio), scale])

    edge, field = shape(4 * LV, LN), shape(LV, RX, LN)
    press, east, north, mid, outer, cols = call(
        join_kernel, [field, field, field, edge, edge, edge], [own, got]
    )
    wind = None
    for substep in range(ITERS):
        first, last = substep == 0, substep == ITERS - 1
        left = lax.ppermute(cols, "gy", east_ring)
        right = lax.ppermute(cols, "gy", west_ring)
        outer_in = lax.ppermute(outer, ("gx", "gz"), outward)
        mid_in = lax.ppermute(mid, "gz", swap)
        if first:
            wind, geo = call(join_wind_kernel, [field, field], [own_wind, got_wind])
        args = [press, east, north, wind, geo, mass, rate, scale, up, down, mid_in, outer_in, left, right, cols]
        if not first:
            args += [east_edge, north_edge]
        east, north, east_edge, north_edge, star, forced, to_next, to_far, to_prev = stage_one(first, *args)
        from_prev = lax.ppermute(to_next, "gz", along(1))
        from_next = lax.ppermute(to_prev, "gz", along(3))
        from_far = lax.ppermute(to_far, "gz", along(2))
        if last:
            half = shape(2, HALF, RX, LN)
            own_hor, send_hor = call(sort_winds_kernel, [half, half], [east, north])
            got_hor = lax.ppermute(send_hor, "gz", swap)
            east_after, north_after = merge(own_hor, got_hor)
        results = stage_two(last, star, forced, geo, mass, rate, up, down, from_prev, from_far, from_next)
        if not last:
            wind, geo, press, mid, outer, cols = results
    own_ver, send_ver = results
    got_ver = lax.ppermute(send_ver, "gz", swap)
    vertical_after, geo_after, pressure_after = merge(own_ver, got_ver)
    return east_after, north_after, vertical_after, geo_after, pressure_after


def solution(mesh):
    spec = P("gz", "gx", "gy")
    return jax.shard_map(
        local, mesh=mesh, in_specs=(spec,) * 5 + (P("gx", "gy"),), out_specs=(spec,) * 5, check_vma=False
    )
```

```python
import functools

import jax
import jax.numpy as jnp
from jax import lax
from jax.experimental import pallas as pl
from jax.experimental.pallas import tpu as pltpu
from jax.sharding import PartitionSpec as P


ITERS = 3
GRANT = 64800

horiz_push = 0.25
mass_flux = 0.2
buoy_coupling = 0.5
geo_rate = 0.5
level_flux = 0.5
stiffness = 30.0


F32 = jnp.float32
NZ = 96
LV = 24
HALF = 12
RX = 64
LN = 128
TILES = RX // 8
EDGE = 2 * LV
PART = 2 * HALF
VMEM = pl.BlockSpec(memory_space=pltpu.VMEM)
HBM = pl.BlockSpec(memory_space=pltpu.HBM)
PRESS, EAST, NORTH, WIND, GEO = range(5)


def shape(*dims):
    return jax.ShapeDtypeStruct(dims, F32)


def call(body, outs, args, in_specs=None, scratch=(), cost=4_000_000, out_specs=None, grant=24 * 1024):
    return pl.pallas_call(
        body,
        out_shape=outs,
        in_specs=in_specs or [VMEM] * len(args),
        out_specs=out_specs or [VMEM] * len(outs),
        scratch_shapes=list(scratch),
        cost_estimate=pl.CostEstimate(flops=cost, bytes_accessed=1_000_000, transcendentals=0),
        compiler_params=pltpu.CompilerParams(vmem_limit_bytes=grant * 1024),
    )(*args)


def core_of():
    return lax.rem(lax.axis_index("gz"), 2)


def chip_of():
    return lax.div(lax.axis_index("gz"), 2)


def lanes():
    return lax.broadcasted_iota(jnp.int32, (8, LN), 1)


def roll_lanes(value, amount):
    return pltpu.roll(value, amount % LN, 1)


def rows_at(start):
    return pl.ds(pl.multiple_of(start, 8), 8)


def pack_columns(tile_at, out, base, groups):
    lane = lanes()
    for g in range(groups):
        acc = jnp.zeros((8, LN), F32)
        for j in range(4):
            for t in range(TILES):
                slot = 8 * j + t
                moved = roll_lanes(tile_at(4 * g + j, t), 4 * slot - 126)
                acc = jnp.where(lane // 4 == slot, moved, acc)
        out[base + 8 * g : base + 8 * g + 8, :] = acc


def pack_rows(tile_at, groups):
    firsts, lasts = [], []
    for g in range(groups):
        first = [tile_at(4 * g + j, 0)[0:2] for j in range(4)]
        last = [tile_at(4 * g + j, TILES - 1)[6:8] for j in range(4)]
        firsts.append(jnp.concatenate(first, 0))
        lasts.append(jnp.concatenate(last, 0))
    return firsts, lasts


def tiles_of(ref, *lead):
    return lambda k, t: ref[(*lead, k, slice(8 * t, 8 * t + 8), slice(None))]


def split_kernel(*refs):
    ins, (send, keep, give, whole, part, sem) = refs[:5], refs[5:]
    core = core_of()
    ours = pl.ds(pl.multiple_of(core * RX, RX), RX)
    theirs = pl.ds(pl.multiple_of((1 - core) * RX, RX), RX)
    copies = []
    for f in range(5):
        if f < 3:
            copy = pltpu.make_async_copy(ins[f], whole.at[f], sem.at[f])
        else:
            copy = pltpu.make_async_copy(ins[f].at[:, theirs, :], part.at[f - 3], sem.at[f])
        copy.start()
        copies.append(copy)
    for f in range(5):
        copies[f].wait()
        source = whole.at[f, :, theirs, :] if f < 3 else part.at[f - 3]
        copy = pltpu.make_async_copy(source, send.at[f], sem.at[5 + f])
        copy.start()
        copies.append(copy)

    def half(f, which):
        def tile_at(k, t):
            return whole[f, k, rows_at(which * RX + 8 * t), :]

        return tile_at

    for out, near in ((keep, core), (give, 1 - core)):
        pack_columns(half(PRESS, near), out, 0, 3)
        pack_columns(half(NORTH, near), out, PART, 3)
        for part_at, (which, f) in enumerate(((near, PRESS), (near, EAST), (1 - near, PRESS), (1 - near, EAST))):
            for g, (first, last) in enumerate(zip(*pack_rows(half(f, which), 3))):
                base = (2 + part_at) * PART + 8 * g
                out[base : base + 8, :] = jnp.where(near == 0, first, last)
    for copy in copies[5:]:
        copy.wait()


def split(*fields):
    edges = shape(6 * PART, LN)
    return call(
        split_kernel,
        [shape(5, HALF, RX, LN), edges, edges],
        fields,
        in_specs=[HBM] * 5,
        out_specs=[HBM, VMEM, VMEM],
        scratch=[
            pltpu.VMEM((3, HALF, 2 * RX, LN), F32),
            pltpu.VMEM((2, HALF, RX, LN), F32),
            pltpu.SemaphoreType.DMA((10,)),
        ],
        grant=GRANT,
    )


def edges_kernel(keep, got, cols, outer, mid):
    core = core_of()
    for which, out in enumerate((cols, outer, mid)):
        for f in range(2):
            part = slice((2 * which + f) * PART, (2 * which + f + 1) * PART)
            for piece in range(2):
                at = (2 * f + piece) * PART
                out[at : at + PART, :] = jnp.where(core == piece, keep[part, :], got[part, :])


def merge_kernel(count, own, got, *refs):
    outs, sem = refs[:count], refs[-1]
    if len(refs) > count + 1:
        refs[count][...] = jnp.zeros((8, LN), F32)
    core = core_of()
    copies = []
    for f in range(count):
        for which, src in ((core, own), (1 - core, got)):
            rows = pl.ds(pl.multiple_of(which * RX, RX), RX)
            copy = pltpu.make_async_copy(src.at[f], outs[f].at[:, rows, :], sem.at[len(copies)])
            copy.start()
            copies.append(copy)
    for copy in copies:
        copy.wait()


def merge(own, got, token=False):
    count = own.shape[0]
    return call(
        functools.partial(merge_kernel, count),
        [shape(HALF, 2 * RX, LN)] * count + [shape(8, LN)] * token,
        [own, got],
        out_specs=[HBM] * count + [VMEM] * token,
        scratch=[pltpu.SemaphoreType.DMA((2 * count,))],
    )


def inner_kernel(first, *refs):
    if first:
        ins, (got, mass, east_out, north_out, star, ends) = refs[:3], refs[3:]
    else:
        (press, east, north, wind, geo, mass, east_fix) = refs[:7]
        (east_out, north_out, star, ends, heave, geo_out) = refs[7:]
    core = core_of()
    row = lax.broadcasted_iota(jnp.int32, (8, LN), 0)
    zero = jnp.zeros((8, LN), F32)

    def row_difference(tiles):
        above = [pltpu.roll(tile, 7, 0) for tile in tiles] + [zero]
        below = [zero] + [pltpu.roll(tile, 1, 0) for tile in tiles]
        return [
            jnp.where(row == 7, above[t + 1], above[t]) - jnp.where(row == 0, below[t], below[t + 1])
            for t in range(TILES)
        ]

    def group(g, carry):
        piece = g // 3

        def tile_at(f, k, t):
            tile = slice(8 * t, 8 * t + 8)
            if not first:
                return (press, east, north)[f][k, tile, :]
            k = k - HALF * piece
            return jnp.where(core == piece, ins[f][k, rows_at(core * RX + 8 * t), :], got[f, k, tile, :])

        rows = rows_at(8 * g)
        end_rows = []
        if not first:
            e_fix = east_fix[rows, :]
        for j in range(4):
            k = 4 * g + j
            p = [tile_at(PRESS, k, t) for t in range(TILES)]
            end_rows += [p[0][0:1], p[-1][7:8]]
            e = [tile_at(EAST, k, t) for t in range(TILES)]
            if not first:
                e[0] = e[0] + jnp.where(row == 0, e_fix[2 * j : 2 * j + 1], 0.0)
                e[-1] = e[-1] + jnp.where(row == 7, e_fix[2 * j + 1 : 2 * j + 2], 0.0)
            e = [tile - horiz_push * step for tile, step in zip(e, row_difference(p))]
            spread = row_difference(e)
            for t in range(TILES):
                tile = slice(8 * t, 8 * t + 8)
                east_out[k, tile, :] = e[t]
                n = tile_at(NORTH, k, t)
                n = n - horiz_push * (roll_lanes(p[t], -1) - roll_lanes(p[t], 1))
                north_out[k, tile, :] = n
                divergence = spread[t] + (roll_lanes(n, -1) - roll_lanes(n, 1))
                star[k, tile, :] = p[t] - mass_flux * mass[tile, :] * divergence
                if not first:
                    moved = wind[k + 1, tile, :]
                    geo_now = geo[k, tile, :] + geo_rate * moved
                    geo_out[k, tile, :] = geo_now
                    heave[k, tile, :] = moved + buoy_coupling * geo_now
        ends[rows, :] = jnp.concatenate(end_rows, 0)
        return carry

    lax.fori_loop(0, LV // 4, group, 0)


def inner(first, *args):
    field = shape(LV, RX, LN)
    return call(
        functools.partial(inner_kernel, first),
        [field, field, field, shape(EDGE, LN)] + ([] if first else [field, field]),
        args,
    )


def heave_kernel(wind, geo, got, heave, geo_out):
    core = core_of()
    rows = pl.ds(pl.multiple_of(core * RX, RX), RX)

    def level(k, carry):
        here, there = core * HALF + k, (1 - core) * HALF + k
        geo_out[here] = geo[k, rows, :]
        heave[here] = wind[k, rows, :] + buoy_coupling * geo[k, rows, :]
        geo_out[there] = got[GEO, k]
        heave[there] = got[WIND, k] + buoy_coupling * got[GEO, k]
        return carry

    lax.fori_loop(0, HALF, level, 0)


def rim_kernel(first, last, *refs):
    (star_in, heave, ends, mass, rate, up, down, mid, outer, left, right, own_cols) = refs[:12]
    refs = refs[12:]
    if not first:
        (north_fix_in, east_edge, north_own, north_edge), refs = refs[:4], refs[4:]
    (star, forced, to_next, to_far, to_prev, east_fix, north_fix) = refs[:7]
    if not last:
        east_edge_out, north_own_out, north_edge_out = refs[7:]
    core, chip = core_of(), chip_of()
    lane = lanes()
    quarter = lane % 4
    rim_lane = jnp.logical_or(lane < 2, lane >= LN - 2)
    row = lax.broadcasted_iota(jnp.int32, (8, LN), 0)
    odd = row % 2 == 1
    ratio, inverse, scale = rate[0], rate[1], rate[3]

    for g in range(LV // 4):
        rows = slice(8 * g, 8 * g + 8)
        more = slice(EDGE + 8 * g, EDGE + 8 * g + 8)
        p_low = jnp.where(core == 0, outer[rows, :], mid[rows, :])
        p_high = jnp.where(core == 0, mid[rows, :], outer[rows, :])
        p_edge = jnp.where(quarter < 2, left[rows, :], right[rows, :])
        p_own = own_cols[rows, :]
        if first:
            e_edge = jnp.where(
                odd,
                jnp.where(core == 0, outer[more, :], mid[more, :]),
                jnp.where(core == 0, mid[more, :], outer[more, :]),
            )
            n_own, n_edge = own_cols[more, :], jnp.where(quarter < 2, left[more, :], right[more, :])
        else:
            e_edge, n_own, n_edge = east_edge[rows, :], north_own[rows, :], north_edge[rows, :]
        own_up, own_down = roll_lanes(p_own, -1), roll_lanes(p_own, 1)
        edge_up, edge_down = roll_lanes(p_edge, -1), roll_lanes(p_edge, 1)
        low_side = quarter == 1
        n_edge = n_edge - horiz_push * jnp.where(low_side, own_up - edge_down, edge_up - own_down)
        n_own = n_own - horiz_push * jnp.where(low_side, edge_up - own_down, own_up - edge_down)
        n_fix = -horiz_push * jnp.where(low_side, edge_up - own_up, own_down - edge_down)
        if not first:
            n_fix = n_fix + north_fix_in[rows, :]
        gap = n_edge - (n_own - n_fix)
        north_fix[rows, :] = n_fix
        if not last:
            north_own_out[rows, :] = n_own
            north_edge_out[rows, :] = n_edge
        spread = jnp.where(
            quarter == 0,
            roll_lanes(n_fix, -1),
            jnp.where(
                quarter == 1,
                roll_lanes(gap, -1),
                -jnp.where(quarter == 2, roll_lanes(gap, 1), roll_lanes(n_fix, 1)),
            ),
        )
        tips = ends[rows, :]
        edges, fixes = [], []
        for j in range(4):
            a, b = 2 * j, 2 * j + 1
            over = e_edge[a : a + 1] - horiz_push * (p_high[b : b + 1] - tips[b : b + 1])
            under = e_edge[b : b + 1] - horiz_push * (tips[a : a + 1] - p_low[a : a + 1])
            lift, sink = horiz_push * p_low[b : b + 1], -horiz_push * p_high[a : a + 1]
            edges += [over, under]
            fixes += [lift, sink]
            for t in range(TILES):
                tile = slice(8 * t, 8 * t + 8)
                term = jnp.where(rim_lane, roll_lanes(spread, 126 - 4 * (8 * j + t)), 0.0)
                if t == 0:
                    term = term - jnp.where(row == 0, under, jnp.where(row == 1, lift, 0.0))
                if t == TILES - 1:
                    term = term + jnp.where(row == 7, over, jnp.where(row == 6, sink, 0.0))
                k = 4 * g + j
                star[k, tile, :] = star_in[k, tile, :] - mass_flux * mass[tile, :] * term
        if not last:
            east_edge_out[rows, :] = jnp.concatenate(edges, 0)
        east_fix[rows, :] = jnp.concatenate(fixes, 0)

    for t in range(TILES):
        tile = slice(8 * t, 8 * t + 8)
        rho, inv, factor = ratio[tile], inverse[tile], scale[tile]
        bottom, top = factor * star[0, tile, :], factor * star[LV - 1, tile, :]
        total = -up[0, tile, :] * bottom
        tail = -inv * down[0, tile, :] * bottom
        power = None
        for k in range(LV):
            f = heave[k, tile, :]
            if k < LV - 1:
                f = f - star[k + 1, tile, :]
            if k > 0:
                f = f + star[k - 1, tile, :]
            f = factor * f
            forced[k, tile, :] = f
            total = rho * total + up[k + 1, tile, :] * f
            weighted = down[k + 1, tile, :] * f
            tail = tail + (weighted if k == 0 else power * weighted)
            power = rho if k == 0 else power * rho
        total = total + inv * up[LV + 1, tile, :] * top
        tail = tail + power * (down[LV + 1, tile, :] * top)
        to_next[0, tile, :] = jnp.where(chip < 3, total, tail)
        to_next[1, tile, :] = top
        to_far[tile, :] = jnp.where(chip < 2, total, tail)
        to_prev[0, tile, :] = jnp.where(chip > 0, tail, total)
        to_prev[1, tile, :] = bottom


def rim(first, last, *args):
    edge, field, pair = shape(EDGE, LN), shape(LV, RX, LN), shape(2, RX, LN)
    return call(
        functools.partial(rim_kernel, first, last),
        [field, field, pair, shape(RX, LN), pair] + [edge] * (2 if last else 5),
        args,
    )


def solve_kernel(last, *refs):
    (star, forced, geo, mass, rate, up, down, from_prev, from_far, from_next) = refs[:10]
    refs = refs[10:]
    if last:
        (after, mine, theirs, sums, wind, geo_out, press) = refs
    else:
        (wind, press, mid, outer, cols, sums) = refs
    core, chip = core_of(), chip_of()

    for t in range(TILES):
        tile = slice(8 * t, 8 * t + 8)
        ratio, inverse, deep, scale = (rate[i, tile, :] for i in range(4))
        zero = jnp.zeros((8, LN), F32)
        prev, far, after = from_prev[0, tile, :], from_far[tile, :], from_next[0, tile, :]
        star_under = jnp.where(chip > 0, from_prev[1, tile, :], zero)
        star_over = jnp.where(chip < 3, from_next[1, tile, :], zero)
        far_deep = deep * far
        enter = jnp.where(
            chip == 0,
            zero,
            prev + jnp.where(chip >= 2, far_deep, zero) + jnp.where(chip == 3, deep * deep * after, zero),
        )
        above = jnp.where(
            chip == 3,
            zero,
            after + jnp.where(chip <= 1, far_deep, zero) + jnp.where(chip == 0, deep * deep * prev, zero),
        )
        enter = enter - inverse * up[1, tile, :] * star_under - up[0, tile, :] * (scale * star[0, tile, :])
        above = above + inverse * down[LV, tile, :] * star_over + down[LV + 1, tile, :] * (scale * star[LV - 1, tile, :])

        def force(k):
            f = forced[k, tile, :]
            if k == 0:
                f = f + star_under
            if k == LV - 1:
                f = f - star_over
            return f

        total = enter
        for k in range(LV):
            total = ratio * total + up[k + 1, tile, :] * force(k)
            sums[k, tile, :] = total
        carried = ratio * above
        higher = down[LV + 1, tile, :] * (ratio * total) + up[LV + 1, tile, :] * above
        wind[LV + 1, tile, :] = higher
        flux = level_flux * mass[tile, :]
        here = None
        for k in range(LV - 1, -1, -1):
            solved = down[k + 1, tile, :] * sums[k, tile, :] + up[k + 1, tile, :] * carried
            wind[k + 1, tile, :] = solved
            if last:
                geo_out[k, tile, :] = geo[k, tile, :] + geo_rate * solved
            if k < LV - 1:
                press[k + 1, tile, :] = star[k + 1, tile, :] - flux * (higher - solved)
                higher = here
            here = solved
            carried = ratio * (carried + down[k + 1, tile, :] * force(k))
        lowest = down[0, tile, :] * enter + up[0, tile, :] * carried
        wind[0, tile, :] = lowest
        press[0, tile, :] = star[0, tile, :] - flux * (higher - lowest)

    if last:
        here, there = core * HALF, (1 - core) * HALF
        for k in range(HALF):
            for f, (source, off) in enumerate(((wind, 1), (geo_out, 0), (press, 0))):
                mine[f, k] = source[here + k + off]
                theirs[f, k] = source[there + k + off]
    else:
        for g, (first_rows, last_rows) in enumerate(zip(*pack_rows(tiles_of(press), LV // 4))):
            rows = slice(8 * g, 8 * g + 8)
            mid[rows, :] = jnp.where(core == 0, last_rows, first_rows)
            outer[rows, :] = jnp.where(core == 0, first_rows, last_rows)
        pack_columns(tiles_of(press), cols, 0, LV // 4)


def solve(last, *args):
    edge, field, tall = shape(EDGE, LN), shape(LV, RX, LN), shape(LV + 2, RX, LN)
    if last:
        outs = [shape(3, HALF, RX, LN)] * 2
        scratch = [pltpu.VMEM(s.shape, F32) for s in (field, tall, field, field)]
    else:
        outs = [tall, field, edge, edge, edge]
        scratch = [pltpu.VMEM(field.shape, F32)]
    return call(functools.partial(solve_kernel, last), outs, args, scratch=scratch)


def sort_winds_kernel(east, north, east_fix, north_fix, mine, theirs):
    core = core_of()
    lane = lanes()
    inner_lane = jnp.logical_or(lane == 0, lane == LN - 1)
    row = lax.broadcasted_iota(jnp.int32, (8, LN), 0)

    def group(g, carry):
        for out, piece in ((mine, core), (theirs, 1 - core)):
            rows = rows_at(8 * (3 * piece + g))
            e_fix, n_fix = east_fix[rows, :], north_fix[rows, :]
            for j in range(4):
                k = HALF * piece + 4 * g + j
                for t in range(TILES):
                    tile = slice(8 * t, 8 * t + 8)
                    e, n = east[k, tile, :], north[k, tile, :]
                    if t == 0:
                        e = e + jnp.where(row == 0, e_fix[2 * j : 2 * j + 1], 0.0)
                    if t == TILES - 1:
                        e = e + jnp.where(row == 7, e_fix[2 * j + 1 : 2 * j + 2], 0.0)
                    n = n + jnp.where(inner_lane, roll_lanes(n_fix, 126 - 4 * (8 * j + t)), 0.0)
                    out[0, 4 * g + j, tile, :] = e
                    out[1, 4 * g + j, tile, :] = n
        return carry

    lax.fori_loop(0, 3, group, 0)


def local(east_wind, north_wind, vertical_wind, geopotential, pressure, column_mass):
    columns, tiles, pieces = lax.axis_size("gx"), lax.axis_size("gy"), lax.axis_size("gz")
    core, chip = core_of(), chip_of()
    swap = [(i, i ^ 1) for i in range(pieces)]

    def along(distance):
        return [(i, (i + 2 * distance) % pieces) for i in range(pieces)]

    outward = [
        (a * pieces + z, (a + (1 if z % 2 else -1)) % columns * pieces + (z ^ 1))
        for a in range(columns)
        for z in range(pieces)
    ]
    east_ring = [(i, (i + 1) % tiles) for i in range(tiles)]
    west_ring = [(i, (i - 1) % tiles) for i in range(tiles)]

    fields = (pressure, east_wind, north_wind, vertical_wind, geopotential)
    send, keep, give = split(*fields)
    got_edges = lax.ppermute(give, "gz", swap)
    wide = shape(2 * EDGE, LN)
    send, got_edges = lax.optimization_barrier((send, got_edges))
    got = lax.ppermute(send, "gz", swap)
    cols, outer, mid = call(edges_kernel, [wide] * 3, [keep, got_edges])

    mass = lax.dynamic_slice_in_dim(column_mass, core * RX, RX, 0)
    stiff_ratio = stiffness * mass
    root = jnp.sqrt(1.0 + 4.0 * stiff_ratio)
    ratio = (1.0 + 2.0 * stiff_ratio - root) / (2.0 * stiff_ratio)
    log_ratio = jnp.log(ratio)
    level = (chip * LV - 1 + lax.iota(jnp.int32, LV + 2)).astype(F32)[:, None, None]
    up = 1.0 - jnp.exp((2.0 * (level + 1.0)) * log_ratio)
    down = 1.0 - jnp.exp((2.0 * (NZ - level)) * log_ratio)
    scale = 1.0 / (root * (1.0 - jnp.exp((2.0 * (NZ + 1.0)) * log_ratio)))
    rate = jnp.stack([ratio, 1.0 / ratio, jnp.exp(float(LV) * log_ratio), scale])

    field = shape(LV, RX, LN)
    for substep in range(ITERS):
        first, last = substep == 0, substep == ITERS - 1
        left = lax.ppermute(cols, "gy", east_ring)
        right = lax.ppermute(cols, "gy", west_ring)
        outer_in = lax.ppermute(outer, ("gx", "gz"), outward)
        if first:
            mid_in = mid
            east, north, star, ends = inner(first, *fields[:3], got, mass)
            heave, geo = call(heave_kernel, [field, field], [*fields[3:], got])
        else:
            mid_in = lax.ppermute(mid, "gz", swap)
            east, north, star, ends, heave, geo = inner(first, press, east, north, wind, geo, mass, east_fix)
        args = [star, heave, ends, mass, rate, up, down, mid_in, outer_in, left, right, cols]
        if not first:
            args += [north_fix, *edges]
        star, forced, to_next, to_far, to_prev, east_fix, north_fix, *edges = rim(first, last, *args)
        from_far = lax.ppermute(to_far, "gz", along(2))
        from_prev = lax.ppermute(to_next, "gz", along(1))
        from_next = lax.ppermute(to_prev, "gz", along(3))
        args = [star, forced, geo, mass, rate, up, down, from_prev, from_far, from_next]
        if last:
            half = shape(2, HALF, RX, LN)
            own_hor, send_hor = call(sort_winds_kernel, [half, half], [east, north, east_fix, north_fix])
            got_hor = lax.ppermute(send_hor, "gz", swap)
            east_after, north_after, written = merge(own_hor, got_hor, token=True)
            own_ver, send_ver = solve(last, *args, written)
        else:
            wind, press, mid, outer, cols = solve(last, *args)
    got_ver = lax.ppermute(send_ver, "gz", swap)
    vertical_after, geo_after, pressure_after = merge(own_ver, got_ver)
    return east_after, north_after, vertical_after, geo_after, pressure_after


def solution(mesh):
    spec = P("gz", "gx", "gy")
    return jax.shard_map(
        local, mesh=mesh, in_specs=(spec,) * 5 + (P("gx", "gy"),), out_specs=(spec,) * 5, check_vma=False
    )
```

```python
import functools

import jax
import jax.numpy as jnp
from jax import lax
from jax.experimental import pallas as pl
from jax.experimental.pallas import tpu as pltpu
from jax.sharding import PartitionSpec as P


ITERS = 3
GRANT = 54800

horiz_push = 0.25
mass_flux = 0.2
buoy_coupling = 0.5
geo_rate = 0.5
level_flux = 0.5
stiffness = 30.0


F32 = jnp.float32
NZ = 96
LV = 24
HALF = 12
RX = 64
LN = 128
TILES = RX // 8
EDGE = 2 * LV
PART = 2 * HALF
VMEM = pl.BlockSpec(memory_space=pltpu.VMEM)
HBM = pl.BlockSpec(memory_space=pltpu.HBM)
PRESS, EAST, NORTH, WIND, GEO = range(5)


def shape(*dims):
    return jax.ShapeDtypeStruct(dims, F32)


def call(body, outs, args, in_specs=None, scratch=(), cost=4_000_000, out_specs=None, grant=24 * 1024):
    return pl.pallas_call(
        body,
        out_shape=outs,
        in_specs=in_specs or [VMEM] * len(args),
        out_specs=out_specs or [VMEM] * len(outs),
        scratch_shapes=list(scratch),
        cost_estimate=pl.CostEstimate(flops=cost, bytes_accessed=1_000_000, transcendentals=0),
        compiler_params=pltpu.CompilerParams(vmem_limit_bytes=grant * 1024),
    )(*args)


def core_of():
    return lax.rem(lax.axis_index("gz"), 2)


def chip_of():
    return lax.div(lax.axis_index("gz"), 2)


def lanes():
    return lax.broadcasted_iota(jnp.int32, (8, LN), 1)


def roll_lanes(value, amount):
    return pltpu.roll(value, amount % LN, 1)


def rows_at(start):
    return pl.ds(pl.multiple_of(start, 8), 8)


def pack_columns(groups):
    lane = lanes()
    packed = [jnp.zeros((8, LN), F32)] * len(groups)
    for slot in range(4 * TILES):
        j, t = divmod(slot, TILES)
        here = lane // 4 == slot
        packed = [
            jnp.where(here, roll_lanes(tile_at(k + j, t), 4 * slot - 126), acc)
            for acc, (tile_at, k, _, _) in zip(packed, groups)
        ]
    for acc, (_, _, out, row) in zip(packed, groups):
        out[row : row + 8, :] = acc


def pack_rows(tile_at, groups):
    firsts, lasts = [], []
    for g in range(groups):
        first = [tile_at(4 * g + j, 0)[0:2] for j in range(4)]
        last = [tile_at(4 * g + j, TILES - 1)[6:8] for j in range(4)]
        firsts.append(jnp.concatenate(first, 0))
        lasts.append(jnp.concatenate(last, 0))
    return firsts, lasts


def tiles_of(ref, *lead):
    return lambda k, t: ref[(*lead, k, slice(8 * t, 8 * t + 8), slice(None))]


def split_kernel(*refs):
    ins, (send, keep, give, whole, part, sem) = refs[:5], refs[5:]
    core = core_of()
    ours = pl.ds(pl.multiple_of(core * RX, RX), RX)
    theirs = pl.ds(pl.multiple_of((1 - core) * RX, RX), RX)
    loads, stores = [], []

    def store(f):
        loads[f].wait()
        source = whole.at[f, :, theirs, :] if f < 3 else part.at[f - 3]
        stores.append(pltpu.make_async_copy(source, send.at[f], sem.at[5 + f]))
        stores[-1].start()

    for f in range(5):
        if f < 3:
            loads.append(pltpu.make_async_copy(ins[f], whole.at[f], sem.at[f]))
        else:
            loads.append(pltpu.make_async_copy(ins[f].at[:, theirs, :], part.at[f - 3], sem.at[f]))
        loads[-1].start()
    for f in range(3):
        store(f)

    def half(f, which):
        def tile_at(k, t):
            return whole[f, k, rows_at(which * RX + 8 * t), :]

        return tile_at

    jobs = ((give, 1 - core), (keep, core))
    for out, near in jobs:
        for part_at, (which, f) in enumerate(((near, PRESS), (near, EAST), (1 - near, PRESS), (1 - near, EAST))):
            for g, (first, last) in enumerate(zip(*pack_rows(half(f, which), 3))):
                base = (2 + part_at) * PART + 8 * g
                out[base : base + 8, :] = jnp.where(near == 0, first, last)
    for f in range(3, 5):
        store(f)
    pack_columns(
        [
            (half(f, near), 4 * g, out, i * PART + 8 * g)
            for out, near in jobs
            for i, f in enumerate((PRESS, NORTH))
            for g in range(3)
        ]
    )
    for copy in stores:
        copy.wait()


def split(*fields):
    edges = shape(6 * PART, LN)
    return call(
        split_kernel,
        [shape(5, HALF, RX, LN), edges, edges],
        fields,
        in_specs=[HBM] * 5,
        out_specs=[HBM, VMEM, VMEM],
        scratch=[
            pltpu.VMEM((3, HALF, 2 * RX, LN), F32),
            pltpu.VMEM((2, HALF, RX, LN), F32),
            pltpu.SemaphoreType.DMA((10,)),
        ],
        grant=GRANT,
    )


def edges_kernel(keep, got, cols, outer, mid):
    core = core_of()
    for which, out in enumerate((cols, outer, mid)):
        for f in range(2):
            part = slice((2 * which + f) * PART, (2 * which + f + 1) * PART)
            for piece in range(2):
                at = (2 * f + piece) * PART
                out[at : at + PART, :] = jnp.where(core == piece, keep[part, :], got[part, :])


def winds_out_kernel(own, got, east, north, sem):
    core = core_of()
    copies = []
    for f, out in enumerate((east, north)):
        for which, src in ((core, own), (1 - core, got)):
            rows = pl.ds(pl.multiple_of(which * RX, RX), RX)
            copy = pltpu.make_async_copy(src.at[f], out.at[:, rows, :], sem.at[len(copies)])
            copy.start()
            copies.append(copy)
    for copy in copies:
        copy.wait()


def solved_out_kernel(own, got, got_wind, mass, wind, geo, press, fill, sem):
    core = core_of()
    copies = []

    def write(source, out, which):
        rows = pl.ds(pl.multiple_of(which * RX, RX), RX)
        copies.append(pltpu.make_async_copy(source, out.at[:, rows, :], sem.at[len(copies)]))
        copies[-1].start()

    for f, out in enumerate((wind, geo, press)):
        write(own.at[f], out, core)
    write(got_wind.at[pl.ds(1, HALF)], wind, 1 - core)
    flux = level_flux * mass[...]
    for f, out in enumerate((geo, press)):
        for k in range(HALF):
            if f == 0:
                fill[0, k] = got[2, k] + geo_rate * got_wind[k + 1]
            else:
                fill[1, k] = got[3, k] - flux * (got_wind[k + 2] - got_wind[k])
        write(fill.at[f], out, 1 - core)
    for copy in copies:
        copy.wait()


def write_out(body, count, scratch, *args):
    return call(
        body,
        [shape(HALF, 2 * RX, LN)] * count,
        args,
        out_specs=[HBM] * count,
        scratch=[*scratch, pltpu.SemaphoreType.DMA((2 * count,))],
    )


def inner_kernel(first, *refs):
    if first:
        ins, (got, mass, east_out, north_out, star, ends) = refs[:3], refs[3:]
    else:
        (press, east, north, wind, geo, mass, east_fix) = refs[:7]
        (east_out, north_out, star, ends, heave, geo_out) = refs[7:]
    core = core_of()
    row = lax.broadcasted_iota(jnp.int32, (8, LN), 0)
    zero = jnp.zeros((8, LN), F32)

    def row_difference(tiles):
        above = [pltpu.roll(tile, 7, 0) for tile in tiles] + [zero]
        below = [zero] + [pltpu.roll(tile, 1, 0) for tile in tiles]
        return [
            jnp.where(row == 7, above[t + 1], above[t]) - jnp.where(row == 0, below[t], below[t + 1])
            for t in range(TILES)
        ]

    def group(g, carry):
        piece = g // 3

        def tile_at(f, k, t):
            tile = slice(8 * t, 8 * t + 8)
            if not first:
                return (press, east, north)[f][k, tile, :]
            k = k - HALF * piece
            return jnp.where(core == piece, ins[f][k, rows_at(core * RX + 8 * t), :], got[f, k, tile, :])

        rows = rows_at(8 * g)
        end_rows = []
        if not first:
            e_fix = east_fix[rows, :]
        for j in range(4):
            k = 4 * g + j
            p = [tile_at(PRESS, k, t) for t in range(TILES)]
            end_rows += [p[0][0:1], p[-1][7:8]]
            e = [tile_at(EAST, k, t) for t in range(TILES)]
            if not first:
                e[0] = e[0] + jnp.where(row == 0, e_fix[2 * j : 2 * j + 1], 0.0)
                e[-1] = e[-1] + jnp.where(row == 7, e_fix[2 * j + 1 : 2 * j + 2], 0.0)
            e = [tile - horiz_push * step for tile, step in zip(e, row_difference(p))]
            spread = row_difference(e)
            for t in range(TILES):
                tile = slice(8 * t, 8 * t + 8)
                east_out[k, tile, :] = e[t]
                n = tile_at(NORTH, k, t)
                n = n - horiz_push * (roll_lanes(p[t], -1) - roll_lanes(p[t], 1))
                north_out[k, tile, :] = n
                divergence = spread[t] + (roll_lanes(n, -1) - roll_lanes(n, 1))
                star[k, tile, :] = p[t] - mass_flux * mass[tile, :] * divergence
                if not first:
                    moved = wind[k + 1, tile, :]
                    geo_now = geo[k, tile, :] + geo_rate * moved
                    geo_out[k, tile, :] = geo_now
                    heave[k, tile, :] = moved + buoy_coupling * geo_now
        ends[rows, :] = jnp.concatenate(end_rows, 0)
        return carry

    lax.fori_loop(0, LV // 4, group, 0)


def inner(first, *args):
    field = shape(LV, RX, LN)
    return call(
        functools.partial(inner_kernel, first),
        [field, field, field, shape(EDGE, LN)] + ([] if first else [field, field]),
        args,
    )


def heave_kernel(wind, geo, got, after, heave, geo_out):
    core = core_of()
    rows = pl.ds(pl.multiple_of(core * RX, RX), RX)

    def level(k, carry):
        here, there = core * HALF + k, (1 - core) * HALF + k
        geo_out[here] = geo[k, rows, :]
        heave[here] = wind[k, rows, :] + buoy_coupling * geo[k, rows, :]
        geo_out[there] = got[GEO, k]
        heave[there] = got[WIND, k] + buoy_coupling * got[GEO, k]
        return carry

    lax.fori_loop(0, HALF, level, 0)


def rim_kernel(first, last, *refs):
    (star_in, heave, ends, mass, rate, up, down, mid, outer, left, right, own_cols) = refs[:12]
    refs = refs[12:]
    if not first:
        (north_fix_in, east_edge, north_own, north_edge), refs = refs[:4], refs[4:]
    (star, forced, to_next, to_far, to_prev, east_fix, north_fix) = refs[:7]
    if not last:
        east_edge_out, north_own_out, north_edge_out = refs[7:]
    core, chip = core_of(), chip_of()
    lane = lanes()
    quarter = lane % 4
    rim_lane = jnp.logical_or(lane < 2, lane >= LN - 2)
    row = lax.broadcasted_iota(jnp.int32, (8, LN), 0)
    odd = row % 2 == 1
    ratio, inverse, scale = rate[0], rate[1], rate[3]

    for g in range(LV // 4):
        rows = slice(8 * g, 8 * g + 8)
        more = slice(EDGE + 8 * g, EDGE + 8 * g + 8)
        p_low = jnp.where(core == 0, outer[rows, :], mid[rows, :])
        p_high = jnp.where(core == 0, mid[rows, :], outer[rows, :])
        p_edge = jnp.where(quarter < 2, left[rows, :], right[rows, :])
        p_own = own_cols[rows, :]
        if first:
            e_edge = jnp.where(
                odd,
                jnp.where(core == 0, outer[more, :], mid[more, :]),
                jnp.where(core == 0, mid[more, :], outer[more, :]),
            )
            n_own, n_edge = own_cols[more, :], jnp.where(quarter < 2, left[more, :], right[more, :])
        else:
            e_edge, n_own, n_edge = east_edge[rows, :], north_own[rows, :], north_edge[rows, :]
        own_up, own_down = roll_lanes(p_own, -1), roll_lanes(p_own, 1)
        edge_up, edge_down = roll_lanes(p_edge, -1), roll_lanes(p_edge, 1)
        low_side = quarter == 1
        n_edge = n_edge - horiz_push * jnp.where(low_side, own_up - edge_down, edge_up - own_down)
        n_own = n_own - horiz_push * jnp.where(low_side, edge_up - own_down, own_up - edge_down)
        n_fix = -horiz_push * jnp.where(low_side, edge_up - own_up, own_down - edge_down)
        if not first:
            n_fix = n_fix + north_fix_in[rows, :]
        gap = n_edge - (n_own - n_fix)
        north_fix[rows, :] = n_fix
        if not last:
            north_own_out[rows, :] = n_own
            north_edge_out[rows, :] = n_edge
        spread = jnp.where(
            quarter == 0,
            roll_lanes(n_fix, -1),
            jnp.where(
                quarter == 1,
                roll_lanes(gap, -1),
                -jnp.where(quarter == 2, roll_lanes(gap, 1), roll_lanes(n_fix, 1)),
            ),
        )
        tips = ends[rows, :]
        edges, fixes = [], []
        for j in range(4):
            a, b = 2 * j, 2 * j + 1
            over = e_edge[a : a + 1] - horiz_push * (p_high[b : b + 1] - tips[b : b + 1])
            under = e_edge[b : b + 1] - horiz_push * (tips[a : a + 1] - p_low[a : a + 1])
            lift, sink = horiz_push * p_low[b : b + 1], -horiz_push * p_high[a : a + 1]
            edges += [over, under]
            fixes += [lift, sink]
            for t in range(TILES):
                tile = slice(8 * t, 8 * t + 8)
                term = jnp.where(rim_lane, roll_lanes(spread, 126 - 4 * (8 * j + t)), 0.0)
                if t == 0:
                    term = term - jnp.where(row == 0, under, jnp.where(row == 1, lift, 0.0))
                if t == TILES - 1:
                    term = term + jnp.where(row == 7, over, jnp.where(row == 6, sink, 0.0))
                k = 4 * g + j
                star[k, tile, :] = star_in[k, tile, :] - mass_flux * mass[tile, :] * term
        if not last:
            east_edge_out[rows, :] = jnp.concatenate(edges, 0)
        east_fix[rows, :] = jnp.concatenate(fixes, 0)

    for t in range(TILES):
        tile = slice(8 * t, 8 * t + 8)
        rho, inv, factor = ratio[tile], inverse[tile], scale[tile]
        bottom, top = factor * star[0, tile, :], factor * star[LV - 1, tile, :]
        total = -up[0, tile, :] * bottom
        tail = -inv * down[0, tile, :] * bottom
        power = None
        for k in range(LV):
            f = heave[k, tile, :]
            if k < LV - 1:
                f = f - star[k + 1, tile, :]
            if k > 0:
                f = f + star[k - 1, tile, :]
            f = factor * f
            forced[k, tile, :] = f
            total = rho * total + up[k + 1, tile, :] * f
            weighted = down[k + 1, tile, :] * f
            tail = tail + (weighted if k == 0 else power * weighted)
            power = rho if k == 0 else power * rho
        total = total + inv * up[LV + 1, tile, :] * top
        tail = tail + power * (down[LV + 1, tile, :] * top)
        to_next[0, tile, :] = jnp.where(chip < 3, total, tail)
        to_next[1, tile, :] = top
        to_far[tile, :] = jnp.where(chip < 2, total, tail)
        to_prev[0, tile, :] = jnp.where(chip > 0, tail, total)
        to_prev[1, tile, :] = bottom


def rim(first, last, *args):
    edge, field, pair = shape(EDGE, LN), shape(LV, RX, LN), shape(2, RX, LN)
    return call(
        functools.partial(rim_kernel, first, last),
        [field, field, pair, shape(RX, LN), pair] + [edge] * (2 if last else 5),
        args,
    )


def solve_kernel(last, *refs):
    (star, forced, geo, mass, rate, up, down, from_prev, from_far, from_next) = refs[:10]
    refs = refs[10:]
    if last:
        (mine, wind_theirs, sums, wind, geo_out, press) = refs
    else:
        (wind, press, mid, outer, cols, sums) = refs
    core, chip = core_of(), chip_of()

    for t in range(TILES):
        tile = slice(8 * t, 8 * t + 8)
        ratio, inverse, deep, scale = (rate[i, tile, :] for i in range(4))
        zero = jnp.zeros((8, LN), F32)
        prev, far, after = from_prev[0, tile, :], from_far[tile, :], from_next[0, tile, :]
        star_under = jnp.where(chip > 0, from_prev[1, tile, :], zero)
        star_over = jnp.where(chip < 3, from_next[1, tile, :], zero)
        far_deep = deep * far
        enter = jnp.where(
            chip == 0,
            zero,
            prev + jnp.where(chip >= 2, far_deep, zero) + jnp.where(chip == 3, deep * deep * after, zero),
        )
        above = jnp.where(
            chip == 3,
            zero,
            after + jnp.where(chip <= 1, far_deep, zero) + jnp.where(chip == 0, deep * deep * prev, zero),
        )
        enter = enter - inverse * up[1, tile, :] * star_under - up[0, tile, :] * (scale * star[0, tile, :])
        above = above + inverse * down[LV, tile, :] * star_over + down[LV + 1, tile, :] * (scale * star[LV - 1, tile, :])

        def force(k):
            f = forced[k, tile, :]
            if k == 0:
                f = f + star_under
            if k == LV - 1:
                f = f - star_over
            return f

        total = enter
        for k in range(LV):
            total = ratio * total + up[k + 1, tile, :] * force(k)
            sums[k, tile, :] = total
        carried = ratio * above
        higher = down[LV + 1, tile, :] * (ratio * total) + up[LV + 1, tile, :] * above
        wind[LV + 1, tile, :] = higher
        flux = level_flux * mass[tile, :]
        here = None
        for k in range(LV - 1, -1, -1):
            solved = down[k + 1, tile, :] * sums[k, tile, :] + up[k + 1, tile, :] * carried
            wind[k + 1, tile, :] = solved
            if last:
                geo_out[k, tile, :] = geo[k, tile, :] + geo_rate * solved
            if k < LV - 1:
                press[k + 1, tile, :] = star[k + 1, tile, :] - flux * (higher - solved)
                higher = here
            here = solved
            carried = ratio * (carried + down[k + 1, tile, :] * force(k))
        lowest = down[0, tile, :] * enter + up[0, tile, :] * carried
        wind[0, tile, :] = lowest
        press[0, tile, :] = star[0, tile, :] - flux * (higher - lowest)

    if last:
        here, there = core * HALF, (1 - core) * HALF
        for k in range(HALF):
            for f, (source, off) in enumerate(((wind, 1), (geo_out, 0), (press, 0))):
                mine[f, k] = source[here + k + off]
        for k in range(HALF + 2):
            wind_theirs[k] = wind[there + k]
    else:
        for g, (first_rows, last_rows) in enumerate(zip(*pack_rows(tiles_of(press), LV // 4))):
            rows = slice(8 * g, 8 * g + 8)
            mid[rows, :] = jnp.where(core == 0, last_rows, first_rows)
            outer[rows, :] = jnp.where(core == 0, first_rows, last_rows)
        pack_columns([(tiles_of(press), 4 * g, cols, 8 * g) for g in range(LV // 4)])


def solve(last, *args):
    edge, field, tall = shape(EDGE, LN), shape(LV, RX, LN), shape(LV + 2, RX, LN)
    if last:
        outs = [shape(3, HALF, RX, LN), shape(HALF + 2, RX, LN)]
        scratch = [pltpu.VMEM(s.shape, F32) for s in (field, tall, field, field)]
    else:
        outs = [tall, field, edge, edge, edge]
        scratch = [pltpu.VMEM(field.shape, F32)]
    return call(functools.partial(solve_kernel, last), outs, args, scratch=scratch)


def sort_kernel(east, north, east_fix, north_fix, geo, star, mine, theirs):
    core = core_of()
    lane = lanes()
    inner_lane = jnp.logical_or(lane == 0, lane == LN - 1)
    row = lax.broadcasted_iota(jnp.int32, (8, LN), 0)

    def group(g, carry):
        for out, piece in ((mine, core), (theirs, 1 - core)):
            rows = rows_at(8 * (3 * piece + g))
            e_fix, n_fix = east_fix[rows, :], north_fix[rows, :]
            for j in range(4):
                k = HALF * piece + 4 * g + j
                for t in range(TILES):
                    tile = slice(8 * t, 8 * t + 8)
                    e, n = east[k, tile, :], north[k, tile, :]
                    if t == 0:
                        e = e + jnp.where(row == 0, e_fix[2 * j : 2 * j + 1], 0.0)
                    if t == TILES - 1:
                        e = e + jnp.where(row == 7, e_fix[2 * j + 1 : 2 * j + 2], 0.0)
                    n = n + jnp.where(inner_lane, roll_lanes(n_fix, 126 - 4 * (8 * j + t)), 0.0)
                    out[0, 4 * g + j, tile, :] = e
                    out[1, 4 * g + j, tile, :] = n
                if out is theirs:
                    out[2, 4 * g + j] = geo[k]
                    out[3, 4 * g + j] = star[k]
        return carry

    lax.fori_loop(0, 3, group, 0)


def local(east_wind, north_wind, vertical_wind, geopotential, pressure, column_mass):
    columns, tiles, pieces = lax.axis_size("gx"), lax.axis_size("gy"), lax.axis_size("gz")
    core, chip = core_of(), chip_of()
    swap = [(i, i ^ 1) for i in range(pieces)]

    def along(distance):
        return [(i, (i + 2 * distance) % pieces) for i in range(pieces)]

    outward = [
        (a * pieces + z, (a + (1 if z % 2 else -1)) % columns * pieces + (z ^ 1))
        for a in range(columns)
        for z in range(pieces)
    ]
    east_ring = [(i, (i + 1) % tiles) for i in range(tiles)]
    west_ring = [(i, (i - 1) % tiles) for i in range(tiles)]

    fields = (pressure, east_wind, north_wind, vertical_wind, geopotential)
    send, keep, give = split(*fields)
    got_edges = lax.ppermute(give, "gz", swap)
    wide = shape(2 * EDGE, LN)
    send, got_edges = lax.optimization_barrier((send, got_edges))
    got = lax.ppermute(send, "gz", swap)
    cols, outer, mid = call(edges_kernel, [wide] * 3, [keep, got_edges])

    mass = lax.dynamic_slice_in_dim(column_mass, core * RX, RX, 0)
    stiff_ratio = stiffness * mass
    root = jnp.sqrt(1.0 + 4.0 * stiff_ratio)
    ratio = (1.0 + 2.0 * stiff_ratio - root) / (2.0 * stiff_ratio)
    log_ratio = jnp.log(ratio)
    level = (chip * LV - 1 + lax.iota(jnp.int32, LV + 2)).astype(F32)[:, None, None]
    up = 1.0 - jnp.exp((2.0 * (level + 1.0)) * log_ratio)
    down = 1.0 - jnp.exp((2.0 * (NZ - level)) * log_ratio)
    scale = 1.0 / (root * (1.0 - jnp.exp((2.0 * (NZ + 1.0)) * log_ratio)))
    rate = jnp.stack([ratio, 1.0 / ratio, jnp.exp(float(LV) * log_ratio), scale])

    field = shape(LV, RX, LN)
    for substep in range(ITERS):
        first, last = substep == 0, substep == ITERS - 1
        left = lax.ppermute(cols, "gy", east_ring)
        right = lax.ppermute(cols, "gy", west_ring)
        outer_in = lax.ppermute(outer, ("gx", "gz"), outward)
        if first:
            mid_in = mid
            east, north, star, ends = inner(first, *fields[:3], got, mass)
            heave, geo = call(heave_kernel, [field, field], [*fields[3:], got, ends])
        else:
            mid_in = lax.ppermute(mid, "gz", swap)
            east, north, star, ends, heave, geo = inner(first, press, east, north, wind, geo, mass, east_fix)
        args = [star, heave, ends, mass, rate, up, down, mid_in, outer_in, left, right, cols]
        if not first:
            args += [north_fix, *edges]
        star, forced, to_next, to_far, to_prev, east_fix, north_fix, *edges = rim(first, last, *args)
        from_far = lax.ppermute(to_far, "gz", along(2))
        from_prev = lax.ppermute(to_next, "gz", along(1))
        from_next = lax.ppermute(to_prev, "gz", along(3))
        args = [star, forced, geo, mass, rate, up, down, from_prev, from_far, from_next]
        if last:
            own_part, send_part = call(
                sort_kernel,
                [shape(2, HALF, RX, LN), shape(4, HALF, RX, LN)],
                [east, north, east_fix, north_fix, geo, star],
            )
            got_part = lax.ppermute(send_part, "gz", swap)
            solved, send_solved = solve(last, *args)
            got_solved = lax.ppermute(send_solved, "gz", swap)
            winds_after = write_out(winds_out_kernel, 2, (), own_part, got_part)
            other = lax.dynamic_slice_in_dim(column_mass, (1 - core) * RX, RX, 0)
            fill = pltpu.VMEM((2, HALF, RX, LN), F32)
            solved_after = write_out(solved_out_kernel, 3, (fill,), solved, got_part, got_solved, other)
        else:
            wind, press, mid, outer, cols = solve(last, *args)
    return *winds_after, *solved_after


def solution(mesh):
    spec = P("gz", "gx", "gy")
    return jax.shard_map(
        local, mesh=mesh, in_specs=(spec,) * 5 + (P("gx", "gy"),), out_specs=(spec,) * 5, check_vma=False
    )
```

```python
import functools

import jax
import jax.numpy as jnp
from jax import lax
from jax.experimental import pallas as pl
from jax.experimental.pallas import tpu as pltpu
from jax.sharding import PartitionSpec as P


ITERS = 3
GRANT = 54800

horiz_push = 0.25
mass_flux = 0.2
buoy_coupling = 0.5
geo_rate = 0.5
level_flux = 0.5
stiffness = 30.0


F32 = jnp.float32
NZ = 96
LV = 24
HALF = 12
RX = 64
LN = 128
TILES = RX // 8
EDGE = 2 * LV
PART = 2 * HALF
VMEM = pl.BlockSpec(memory_space=pltpu.VMEM)
HBM = pl.BlockSpec(memory_space=pltpu.HBM)
PRESS, EAST, NORTH, WIND, GEO = range(5)


def shape(*dims):
    return jax.ShapeDtypeStruct(dims, F32)


def call(body, outs, args, in_specs=None, scratch=(), cost=4_000_000, out_specs=None, grant=24 * 1024):
    return pl.pallas_call(
        body,
        out_shape=outs,
        in_specs=in_specs or [VMEM] * len(args),
        out_specs=out_specs or [VMEM] * len(outs),
        scratch_shapes=list(scratch),
        cost_estimate=pl.CostEstimate(flops=cost, bytes_accessed=1_000_000, transcendentals=0),
        compiler_params=pltpu.CompilerParams(vmem_limit_bytes=grant * 1024),
    )(*args)


def core_of():
    return lax.rem(lax.axis_index("gz"), 2)


def chip_of():
    return lax.div(lax.axis_index("gz"), 2)


def lanes():
    return lax.broadcasted_iota(jnp.int32, (8, LN), 1)


def roll_lanes(value, amount):
    return pltpu.roll(value, amount % LN, 1)


def rows_at(start):
    return pl.ds(pl.multiple_of(start, 8), 8)


def pack_columns(groups):
    lane = lanes()
    packed = [jnp.zeros((8, LN), F32)] * len(groups)
    for slot in range(4 * TILES):
        j, t = divmod(slot, TILES)
        here = lane // 4 == slot
        packed = [
            jnp.where(here, roll_lanes(tile_at(k + j, t), 4 * slot - 126), acc)
            for acc, (tile_at, k, _, _) in zip(packed, groups)
        ]
    for acc, (_, _, out, row) in zip(packed, groups):
        out[row : row + 8, :] = acc


def pack_rows(tile_at, groups):
    firsts, lasts = [], []
    for g in range(groups):
        first = [tile_at(4 * g + j, 0)[0:2] for j in range(4)]
        last = [tile_at(4 * g + j, TILES - 1)[6:8] for j in range(4)]
        firsts.append(jnp.concatenate(first, 0))
        lasts.append(jnp.concatenate(last, 0))
    return firsts, lasts


def tiles_of(ref, *lead):
    return lambda k, t: ref[(*lead, k, slice(8 * t, 8 * t + 8), slice(None))]


def split_kernel(*refs):
    ins, (send, keep, give, whole, part, sem) = refs[:5], refs[5:]
    core = core_of()
    ours = pl.ds(pl.multiple_of(core * RX, RX), RX)
    theirs = pl.ds(pl.multiple_of((1 - core) * RX, RX), RX)
    loads, stores = [], []

    def store(f):
        loads[f].wait()
        source = whole.at[f, :, theirs, :] if f < 3 else part.at[f - 3]
        stores.append(pltpu.make_async_copy(source, send.at[f], sem.at[5 + f]))
        stores[-1].start()

    for f in range(5):
        if f < 3:
            loads.append(pltpu.make_async_copy(ins[f], whole.at[f], sem.at[f]))
        else:
            loads.append(pltpu.make_async_copy(ins[f].at[:, theirs, :], part.at[f - 3], sem.at[f]))
        loads[-1].start()
    for f in range(3):
        store(f)

    def half(f, which):
        def tile_at(k, t):
            return whole[f, k, rows_at(which * RX + 8 * t), :]

        return tile_at

    jobs = ((give, 1 - core), (keep, core))
    for out, near in jobs:
        for part_at, (which, f) in enumerate(((near, PRESS), (near, EAST), (1 - near, PRESS), (1 - near, EAST))):
            for g, (first, last) in enumerate(zip(*pack_rows(half(f, which), 3))):
                base = (2 + part_at) * PART + 8 * g
                out[base : base + 8, :] = jnp.where(near == 0, first, last)
    for f in range(3, 5):
        store(f)
    pack_columns(
        [
            (half(f, near), 4 * g, out, i * PART + 8 * g)
            for out, near in jobs
            for i, f in enumerate((PRESS, NORTH))
            for g in range(3)
        ]
    )
    for copy in stores:
        copy.wait()


def split(*fields):
    edges = shape(6 * PART, LN)
    return call(
        split_kernel,
        [shape(5, HALF, RX, LN), edges, edges],
        fields,
        in_specs=[HBM] * 5,
        out_specs=[HBM, VMEM, VMEM],
        scratch=[
            pltpu.VMEM((3, HALF, 2 * RX, LN), F32),
            pltpu.VMEM((2, HALF, RX, LN), F32),
            pltpu.SemaphoreType.DMA((10,)),
        ],
        grant=GRANT,
    )


def edges_kernel(keep, got, cols, outer, mid):
    core = core_of()
    for which, out in enumerate((cols, outer, mid)):
        for f in range(2):
            part = slice((2 * which + f) * PART, (2 * which + f + 1) * PART)
            for piece in range(2):
                at = (2 * f + piece) * PART
                out[at : at + PART, :] = jnp.where(core == piece, keep[part, :], got[part, :])


def winds_out_kernel(own, got, east, north, sem):
    core = core_of()
    copies = []
    for f, out in enumerate((east, north)):
        for which, src in ((core, own), (1 - core, got)):
            rows = pl.ds(pl.multiple_of(which * RX, RX), RX)
            copy = pltpu.make_async_copy(src.at[f], out.at[:, rows, :], sem.at[len(copies)])
            copy.start()
            copies.append(copy)
    for copy in copies:
        copy.wait()


def solved_out_kernel(own, got, got_wind, mass, wind, geo, press, fill, sem):
    core = core_of()
    copies = []

    def write(source, out, which):
        rows = pl.ds(pl.multiple_of(which * RX, RX), RX)
        copies.append(pltpu.make_async_copy(source, out.at[:, rows, :], sem.at[len(copies)]))
        copies[-1].start()

    for f, out in enumerate((wind, geo, press)):
        write(own.at[f], out, core)
    write(got_wind.at[pl.ds(1, HALF)], wind, 1 - core)
    flux = level_flux * mass[...]
    for f, out in enumerate((geo, press)):
        for k in range(HALF):
            if f == 0:
                fill[0, k] = got[2, k] + geo_rate * got_wind[k + 1]
            else:
                fill[1, k] = got[3, k] - flux * (got_wind[k + 2] - got_wind[k])
        write(fill.at[f], out, 1 - core)
    for copy in copies:
        copy.wait()


def write_out(body, count, scratch, *args):
    return call(
        body,
        [shape(HALF, 2 * RX, LN)] * count,
        args,
        out_specs=[HBM] * count,
        scratch=[*scratch, pltpu.SemaphoreType.DMA((2 * count,))],
    )


def inner_kernel(first, *refs):
    if first:
        ins, (got, mass, east_out, north_out, star, ends) = refs[:3], refs[3:]
    else:
        (press, east, north, wind, geo, mass, east_fix) = refs[:7]
        (east_out, north_out, star, ends, heave, geo_out) = refs[7:]
    core = core_of()
    row = lax.broadcasted_iota(jnp.int32, (8, LN), 0)
    zero = jnp.zeros((8, LN), F32)

    def row_difference(tiles):
        above = [pltpu.roll(tile, 7, 0) for tile in tiles] + [zero]
        below = [zero] + [pltpu.roll(tile, 1, 0) for tile in tiles]
        return [
            jnp.where(row == 7, above[t + 1], above[t]) - jnp.where(row == 0, below[t], below[t + 1])
            for t in range(TILES)
        ]

    def group(g, carry):
        piece = g // 3

        def tile_at(f, k, t):
            tile = slice(8 * t, 8 * t + 8)
            if not first:
                return (press, east, north)[f][k, tile, :]
            k = k - HALF * piece
            return jnp.where(core == piece, ins[f][k, rows_at(core * RX + 8 * t), :], got[f, k, tile, :])

        rows = rows_at(8 * g)
        end_rows = []
        if not first:
            e_fix = east_fix[rows, :]
        for j in range(4):
            k = 4 * g + j
            p = [tile_at(PRESS, k, t) for t in range(TILES)]
            end_rows += [p[0][0:1], p[-1][7:8]]
            e = [tile_at(EAST, k, t) for t in range(TILES)]
            if not first:
                e[0] = e[0] + jnp.where(row == 0, e_fix[2 * j : 2 * j + 1], 0.0)
                e[-1] = e[-1] + jnp.where(row == 7, e_fix[2 * j + 1 : 2 * j + 2], 0.0)
            e = [tile - horiz_push * step for tile, step in zip(e, row_difference(p))]
            spread = row_difference(e)
            for t in range(TILES):
                tile = slice(8 * t, 8 * t + 8)
                east_out[k, tile, :] = e[t]
                n = tile_at(NORTH, k, t)
                n = n - horiz_push * (roll_lanes(p[t], -1) - roll_lanes(p[t], 1))
                north_out[k, tile, :] = n
                divergence = spread[t] + (roll_lanes(n, -1) - roll_lanes(n, 1))
                star[k, tile, :] = p[t] - mass_flux * mass[tile, :] * divergence
                if not first:
                    moved = wind[k + 1, tile, :]
                    geo_now = geo[k, tile, :] + geo_rate * moved
                    geo_out[k, tile, :] = geo_now
                    heave[k, tile, :] = moved + buoy_coupling * geo_now
        ends[rows, :] = jnp.concatenate(end_rows, 0)
        return carry

    lax.fori_loop(0, LV // 4, group, 0)


def inner(first, *args):
    field = shape(LV, RX, LN)
    return call(
        functools.partial(inner_kernel, first),
        [field, field, field, shape(EDGE, LN)] + ([] if first else [field, field]),
        args,
    )


def heave_kernel(wind, geo, got, after, heave, geo_out):
    core = core_of()
    rows = pl.ds(pl.multiple_of(core * RX, RX), RX)

    def level(k, carry):
        here, there = core * HALF + k, (1 - core) * HALF + k
        geo_out[here] = geo[k, rows, :]
        heave[here] = wind[k, rows, :] + buoy_coupling * geo[k, rows, :]
        geo_out[there] = got[GEO, k]
        heave[there] = got[WIND, k] + buoy_coupling * got[GEO, k]
        return carry

    lax.fori_loop(0, HALF, level, 0)


def rim_kernel(first, last, *refs):
    (star_in, heave, ends, mass, rate, up, down, mid, outer, across, around, own_cols) = refs[:12]
    refs = refs[12:]
    if not first:
        (north_fix_in, east_edge, north_own, north_edge), refs = refs[:4], refs[4:]
    (star, forced, to_across, to_far, to_around, east_fix, north_fix) = refs[:7]
    if not last:
        east_edge_out, north_own_out, north_edge_out = refs[7:]
    core, chip = core_of(), chip_of()
    lane = lanes()
    quarter = lane % 4
    second = (quarter < 2) == (lax.rem(lax.axis_index("gy"), 2) == 0)
    rim_lane = jnp.logical_or(lane < 2, lane >= LN - 2)
    row = lax.broadcasted_iota(jnp.int32, (8, LN), 0)
    odd = row % 2 == 1
    ratio, inverse, scale = rate[0], rate[1], rate[3]

    for g in range(LV // 4):
        rows = slice(8 * g, 8 * g + 8)
        more = slice(EDGE + 8 * g, EDGE + 8 * g + 8)
        p_low = jnp.where(core == 0, outer[rows, :], mid[rows, :])
        p_high = jnp.where(core == 0, mid[rows, :], outer[rows, :])
        p_edge = jnp.where(second, around[rows, :], across[rows, :])
        p_own = own_cols[rows, :]
        if first:
            e_edge = jnp.where(
                odd,
                jnp.where(core == 0, outer[more, :], mid[more, :]),
                jnp.where(core == 0, mid[more, :], outer[more, :]),
            )
            n_own, n_edge = own_cols[more, :], jnp.where(second, around[more, :], across[more, :])
        else:
            e_edge, n_own, n_edge = east_edge[rows, :], north_own[rows, :], north_edge[rows, :]
        own_up, own_down = roll_lanes(p_own, -1), roll_lanes(p_own, 1)
        edge_up, edge_down = roll_lanes(p_edge, -1), roll_lanes(p_edge, 1)
        low_side = quarter == 1
        n_edge = n_edge - horiz_push * jnp.where(low_side, own_up - edge_down, edge_up - own_down)
        n_own = n_own - horiz_push * jnp.where(low_side, edge_up - own_down, own_up - edge_down)
        n_fix = -horiz_push * jnp.where(low_side, edge_up - own_up, own_down - edge_down)
        if not first:
            n_fix = n_fix + north_fix_in[rows, :]
        gap = n_edge - (n_own - n_fix)
        north_fix[rows, :] = n_fix
        if not last:
            north_own_out[rows, :] = n_own
            north_edge_out[rows, :] = n_edge
        spread = jnp.where(
            quarter == 0,
            roll_lanes(n_fix, -1),
            jnp.where(
                quarter == 1,
                roll_lanes(gap, -1),
                -jnp.where(quarter == 2, roll_lanes(gap, 1), roll_lanes(n_fix, 1)),
            ),
        )
        tips = ends[rows, :]
        edges, fixes = [], []
        for j in range(4):
            a, b = 2 * j, 2 * j + 1
            over = e_edge[a : a + 1] - horiz_push * (p_high[b : b + 1] - tips[b : b + 1])
            under = e_edge[b : b + 1] - horiz_push * (tips[a : a + 1] - p_low[a : a + 1])
            lift, sink = horiz_push * p_low[b : b + 1], -horiz_push * p_high[a : a + 1]
            edges += [over, under]
            fixes += [lift, sink]
            for t in range(TILES):
                tile = slice(8 * t, 8 * t + 8)
                term = jnp.where(rim_lane, roll_lanes(spread, 126 - 4 * (8 * j + t)), 0.0)
                if t == 0:
                    term = term - jnp.where(row == 0, under, jnp.where(row == 1, lift, 0.0))
                if t == TILES - 1:
                    term = term + jnp.where(row == 7, over, jnp.where(row == 6, sink, 0.0))
                k = 4 * g + j
                star[k, tile, :] = star_in[k, tile, :] - mass_flux * mass[tile, :] * term
        if not last:
            east_edge_out[rows, :] = jnp.concatenate(edges, 0)
        east_fix[rows, :] = jnp.concatenate(fixes, 0)

    for t in range(TILES):
        tile = slice(8 * t, 8 * t + 8)
        rho, inv, factor = ratio[tile], inverse[tile], scale[tile]
        bottom, top = factor * star[0, tile, :], factor * star[LV - 1, tile, :]
        total = -up[0, tile, :] * bottom
        tail = -inv * down[0, tile, :] * bottom
        power = None
        for k in range(LV):
            f = heave[k, tile, :]
            if k < LV - 1:
                f = f - star[k + 1, tile, :]
            if k > 0:
                f = f + star[k - 1, tile, :]
            f = factor * f
            forced[k, tile, :] = f
            total = rho * total + up[k + 1, tile, :] * f
            weighted = down[k + 1, tile, :] * f
            tail = tail + (weighted if k == 0 else power * weighted)
            power = rho if k == 0 else power * rho
        total = total + inv * up[LV + 1, tile, :] * top
        tail = tail + power * (down[LV + 1, tile, :] * top)
        even = lax.rem(chip, 2) == 0
        low = chip < 2
        to_across[0, tile, :] = jnp.where(even, total, tail)
        to_across[1, tile, :] = jnp.where(even, top, bottom)
        to_around[0, tile, :] = jnp.where(low, total, tail)
        to_around[1, tile, :] = jnp.where(low, top, bottom)
        to_far[tile, :] = jnp.where(low, total, tail)


def rim(first, last, *args):
    edge, field, pair = shape(EDGE, LN), shape(LV, RX, LN), shape(2, RX, LN)
    return call(
        functools.partial(rim_kernel, first, last),
        [field, field, pair, shape(RX, LN), pair] + [edge] * (2 if last else 5),
        args,
    )


def solve_kernel(last, *refs):
    (star, forced, geo, mass, rate, up, down, from_across, from_far, from_around) = refs[:10]
    refs = refs[10:]
    if last:
        (mine, wind_theirs, sums, wind, geo_out, press) = refs
    else:
        (wind, press, mid, outer, cols, sums) = refs
    core, chip = core_of(), chip_of()

    for t in range(TILES):
        tile = slice(8 * t, 8 * t + 8)
        ratio, inverse, deep, scale = (rate[i, tile, :] for i in range(4))
        zero = jnp.zeros((8, LN), F32)
        near, far, turn = from_across[0, tile, :], deep * from_far[tile, :], from_around[0, tile, :]
        even = lax.rem(chip, 2) == 0
        star_near, star_turn = from_across[1, tile, :], from_around[1, tile, :]
        star_under = jnp.where(even, jnp.where(chip == 2, star_turn, zero), star_near)
        star_over = jnp.where(even, star_near, jnp.where(chip == 1, star_turn, zero))
        turn = jnp.where((chip == 0) | (chip == 3), deep * deep * turn, turn)
        enter = jnp.where(even, zero, near) + jnp.where(chip >= 2, far + turn, zero)
        above = jnp.where(even, near, zero) + jnp.where(chip <= 1, far + turn, zero)
        enter = enter - inverse * up[1, tile, :] * star_under - up[0, tile, :] * (scale * star[0, tile, :])
        above = above + inverse * down[LV, tile, :] * star_over + down[LV + 1, tile, :] * (scale * star[LV - 1, tile, :])

        def force(k):
            f = forced[k, tile, :]
            if k == 0:
                f = f + star_under
            if k == LV - 1:
                f = f - star_over
            return f

        total = enter
        for k in range(LV):
            total = ratio * total + up[k + 1, tile, :] * force(k)
            sums[k, tile, :] = total
        carried = ratio * above
        higher = down[LV + 1, tile, :] * (ratio * total) + up[LV + 1, tile, :] * above
        wind[LV + 1, tile, :] = higher
        flux = level_flux * mass[tile, :]
        here = None
        for k in range(LV - 1, -1, -1):
            solved = down[k + 1, tile, :] * sums[k, tile, :] + up[k + 1, tile, :] * carried
            wind[k + 1, tile, :] = solved
            if last:
                geo_out[k, tile, :] = geo[k, tile, :] + geo_rate * solved
            if k < LV - 1:
                press[k + 1, tile, :] = star[k + 1, tile, :] - flux * (higher - solved)
                higher = here
            here = solved
            carried = ratio * (carried + down[k + 1, tile, :] * force(k))
        lowest = down[0, tile, :] * enter + up[0, tile, :] * carried
        wind[0, tile, :] = lowest
        press[0, tile, :] = star[0, tile, :] - flux * (higher - lowest)

    if last:
        here, there = core * HALF, (1 - core) * HALF
        for k in range(HALF):
            for f, (source, off) in enumerate(((wind, 1), (geo_out, 0), (press, 0))):
                mine[f, k] = source[here + k + off]
        for k in range(HALF + 2):
            wind_theirs[k] = wind[there + k]
    else:
        for g, (first_rows, last_rows) in enumerate(zip(*pack_rows(tiles_of(press), LV // 4))):
            rows = slice(8 * g, 8 * g + 8)
            mid[rows, :] = jnp.where(core == 0, last_rows, first_rows)
            outer[rows, :] = jnp.where(core == 0, first_rows, last_rows)
        pack_columns([(tiles_of(press), 4 * g, cols, 8 * g) for g in range(LV // 4)])


def solve(last, *args):
    edge, field, tall = shape(EDGE, LN), shape(LV, RX, LN), shape(LV + 2, RX, LN)
    if last:
        outs = [shape(3, HALF, RX, LN), shape(HALF + 2, RX, LN)]
        scratch = [pltpu.VMEM(s.shape, F32) for s in (field, tall, field, field)]
    else:
        outs = [tall, field, edge, edge, edge]
        scratch = [pltpu.VMEM(field.shape, F32)]
    return call(functools.partial(solve_kernel, last), outs, args, scratch=scratch)


def sort_kernel(east, north, east_fix, north_fix, geo, star, mine, theirs):
    core = core_of()
    lane = lanes()
    inner_lane = jnp.logical_or(lane == 0, lane == LN - 1)
    row = lax.broadcasted_iota(jnp.int32, (8, LN), 0)

    def group(g, carry):
        for out, piece in ((mine, core), (theirs, 1 - core)):
            rows = rows_at(8 * (3 * piece + g))
            e_fix, n_fix = east_fix[rows, :], north_fix[rows, :]
            for j in range(4):
                k = HALF * piece + 4 * g + j
                for t in range(TILES):
                    tile = slice(8 * t, 8 * t + 8)
                    e, n = east[k, tile, :], north[k, tile, :]
                    if t == 0:
                        e = e + jnp.where(row == 0, e_fix[2 * j : 2 * j + 1], 0.0)
                    if t == TILES - 1:
                        e = e + jnp.where(row == 7, e_fix[2 * j + 1 : 2 * j + 2], 0.0)
                    n = n + jnp.where(inner_lane, roll_lanes(n_fix, 126 - 4 * (8 * j + t)), 0.0)
                    out[0, 4 * g + j, tile, :] = e
                    out[1, 4 * g + j, tile, :] = n
                if out is theirs:
                    out[2, 4 * g + j] = geo[k]
                    out[3, 4 * g + j] = star[k]
        return carry

    lax.fori_loop(0, 3, group, 0)


def local(east_wind, north_wind, vertical_wind, geopotential, pressure, column_mass):
    columns, tiles, pieces = lax.axis_size("gx"), lax.axis_size("gy"), lax.axis_size("gz")
    core, chip = core_of(), chip_of()
    swap = [(i, i ^ 1) for i in range(pieces)]

    across_chip = [(i, i ^ 2) for i in range(pieces)]
    around_chip = [(i, (pieces // 2 - 1 - i // 2) * 2 + i % 2) for i in range(pieces)]
    far_chip = [(i, (i + 4) % pieces) for i in range(pieces)]
    outward = [
        (a * pieces + z, (a + (1 if z % 2 else -1)) % columns * pieces + (z ^ 1))
        for a in range(columns)
        for z in range(pieces)
    ]
    across_tile = [(i, i ^ 1) for i in range(tiles)]
    around_tile = [(i, tiles - 1 - i) for i in range(tiles)]
    if tiles != 4 or pieces != 8:
        raise ValueError("sizes")

    fields = (pressure, east_wind, north_wind, vertical_wind, geopotential)
    send, keep, give = split(*fields)
    got_edges = lax.ppermute(give, "gz", swap)
    wide = shape(2 * EDGE, LN)
    send, got_edges = lax.optimization_barrier((send, got_edges))
    got = lax.ppermute(send, "gz", swap)
    cols, outer, mid = call(edges_kernel, [wide] * 3, [keep, got_edges])

    mass = lax.dynamic_slice_in_dim(column_mass, core * RX, RX, 0)
    stiff_ratio = stiffness * mass
    root = jnp.sqrt(1.0 + 4.0 * stiff_ratio)
    ratio = (1.0 + 2.0 * stiff_ratio - root) / (2.0 * stiff_ratio)
    log_ratio = jnp.log(ratio)
    level = (chip * LV - 1 + lax.iota(jnp.int32, LV + 2)).astype(F32)[:, None, None]
    up = 1.0 - jnp.exp((2.0 * (level + 1.0)) * log_ratio)
    down = 1.0 - jnp.exp((2.0 * (NZ - level)) * log_ratio)
    scale = 1.0 / (root * (1.0 - jnp.exp((2.0 * (NZ + 1.0)) * log_ratio)))
    rate = jnp.stack([ratio, 1.0 / ratio, jnp.exp(float(LV) * log_ratio), scale])

    field = shape(LV, RX, LN)
    for substep in range(ITERS):
        first, last = substep == 0, substep == ITERS - 1
        across = lax.ppermute(cols, "gy", across_tile)
        around = lax.ppermute(cols, "gy", around_tile)
        outer_in = lax.ppermute(outer, ("gx", "gz"), outward)
        if first:
            mid_in = mid
            east, north, star, ends = inner(first, *fields[:3], got, mass)
            heave, geo = call(heave_kernel, [field, field], [*fields[3:], got, ends])
        else:
            mid_in = lax.ppermute(mid, "gz", swap)
            east, north, star, ends, heave, geo = inner(first, press, east, north, wind, geo, mass, east_fix)
        args = [star, heave, ends, mass, rate, up, down, mid_in, outer_in, across, around, cols]
        if not first:
            args += [north_fix, *edges]
        star, forced, to_across, to_far, to_around, east_fix, north_fix, *edges = rim(first, last, *args)
        from_far = lax.ppermute(to_far, "gz", far_chip)
        from_across = lax.ppermute(to_across, "gz", across_chip)
        from_around = lax.ppermute(to_around, "gz", around_chip)
        args = [star, forced, geo, mass, rate, up, down, from_across, from_far, from_around]
        if last:
            own_part, send_part = call(
                sort_kernel,
                [shape(2, HALF, RX, LN), shape(4, HALF, RX, LN)],
                [east, north, east_fix, north_fix, geo, star],
            )
            got_part = lax.ppermute(send_part, "gz", swap)
            solved, send_solved = solve(last, *args)
            got_solved = lax.ppermute(send_solved, "gz", swap)
            winds_after = write_out(winds_out_kernel, 2, (), own_part, got_part)
            other = lax.dynamic_slice_in_dim(column_mass, (1 - core) * RX, RX, 0)
            fill = pltpu.VMEM((2, HALF, RX, LN), F32)
            solved_after = write_out(solved_out_kernel, 3, (fill,), solved, got_part, got_solved, other)
        else:
            wind, press, mid, outer, cols = solve(last, *args)
    return *winds_after, *solved_after


def solution(mesh):
    spec = P("gz", "gx", "gy")
    return jax.shard_map(
        local, mesh=mesh, in_specs=(spec,) * 5 + (P("gx", "gy"),), out_specs=(spec,) * 5, check_vma=False
    )
```

```python
import functools

import jax
import jax.numpy as jnp
from jax import lax
from jax.experimental import pallas as pl
from jax.experimental.pallas import tpu as pltpu
from jax.sharding import PartitionSpec as P


ITERS = 3
GRANT = 54800

horiz_push = 0.25
mass_flux = 0.2
buoy_coupling = 0.5
geo_rate = 0.5
level_flux = 0.5
stiffness = 30.0


F32 = jnp.float32
NZ = 96
LV = 24
HALF = 12
RX = 64
LN = 128
TILES = RX // 8
EDGE = 2 * LV
PART = 2 * HALF
VMEM = pl.BlockSpec(memory_space=pltpu.VMEM)
HBM = pl.BlockSpec(memory_space=pltpu.HBM)
PRESS, EAST, NORTH, WIND, GEO = range(5)


def shape(*dims):
    return jax.ShapeDtypeStruct(dims, F32)


def call(body, outs, args, in_specs=None, scratch=(), cost=4_000_000, out_specs=None, grant=24 * 1024):
    return pl.pallas_call(
        body,
        out_shape=outs,
        in_specs=in_specs or [VMEM] * len(args),
        out_specs=out_specs or [VMEM] * len(outs),
        scratch_shapes=list(scratch),
        cost_estimate=pl.CostEstimate(flops=cost, bytes_accessed=1_000_000, transcendentals=0),
        compiler_params=pltpu.CompilerParams(vmem_limit_bytes=grant * 1024),
    )(*args)


def core_of():
    return lax.rem(lax.axis_index("gz"), 2)


def chip_of():
    return lax.div(lax.axis_index("gz"), 2)


def lanes():
    return lax.broadcasted_iota(jnp.int32, (8, LN), 1)


def roll_lanes(value, amount):
    return pltpu.roll(value, amount % LN, 1)


def rows_at(start):
    return pl.ds(pl.multiple_of(start, 8), 8)


def pack_columns(groups):
    lane = lanes()
    packed = [jnp.zeros((8, LN), F32)] * len(groups)
    for slot in range(4 * TILES):
        j, t = divmod(slot, TILES)
        here = lane // 4 == slot
        packed = [
            jnp.where(here, roll_lanes(tile_at(k + j, t), 4 * slot - 126), acc)
            for acc, (tile_at, k, _, _) in zip(packed, groups)
        ]
    for acc, (_, _, out, row) in zip(packed, groups):
        out[row : row + 8, :] = acc


def pack_rows(tile_at, groups):
    firsts, lasts = [], []
    for g in range(groups):
        first = [tile_at(4 * g + j, 0)[0:2] for j in range(4)]
        last = [tile_at(4 * g + j, TILES - 1)[6:8] for j in range(4)]
        firsts.append(jnp.concatenate(first, 0))
        lasts.append(jnp.concatenate(last, 0))
    return firsts, lasts


def tiles_of(ref, *lead):
    return lambda k, t: ref[(*lead, k, slice(8 * t, 8 * t + 8), slice(None))]


def split_kernel(*refs):
    ins, (send, keep, give, whole, part, sem) = refs[:5], refs[5:]
    core = core_of()
    ours = pl.ds(pl.multiple_of(core * RX, RX), RX)
    theirs = pl.ds(pl.multiple_of((1 - core) * RX, RX), RX)
    loads, stores = [], []

    def store(f):
        loads[f].wait()
        source = whole.at[f, :, theirs, :] if f < 3 else part.at[f - 3]
        stores.append(pltpu.make_async_copy(source, send.at[f], sem.at[5 + f]))
        stores[-1].start()

    for f in range(5):
        if f < 3:
            loads.append(pltpu.make_async_copy(ins[f], whole.at[f], sem.at[f]))
        else:
            loads.append(pltpu.make_async_copy(ins[f].at[:, theirs, :], part.at[f - 3], sem.at[f]))
        loads[-1].start()
    for f in range(3):
        store(f)

    def half(f, which):
        def tile_at(k, t):
            return whole[f, k, rows_at(which * RX + 8 * t), :]

        return tile_at

    jobs = ((give, 1 - core), (keep, core))
    for out, near in jobs:
        for part_at, (which, f) in enumerate(((near, PRESS), (near, EAST), (1 - near, PRESS), (1 - near, EAST))):
            for g, (first, last) in enumerate(zip(*pack_rows(half(f, which), 3))):
                base = (2 + part_at) * PART + 8 * g
                out[base : base + 8, :] = jnp.where(near == 0, first, last)
    for f in range(3, 5):
        store(f)
    pack_columns(
        [
            (half(f, near), 4 * g, out, i * PART + 8 * g)
            for out, near in jobs
            for i, f in enumerate((PRESS, NORTH))
            for g in range(3)
        ]
    )
    for copy in stores:
        copy.wait()


def split(*fields):
    edges = shape(6 * PART, LN)
    return call(
        split_kernel,
        [shape(5, HALF, RX, LN), edges, edges],
        fields,
        in_specs=[HBM] * 5,
        out_specs=[HBM, VMEM, VMEM],
        scratch=[
            pltpu.VMEM((3, HALF, 2 * RX, LN), F32),
            pltpu.VMEM((2, HALF, RX, LN), F32),
            pltpu.SemaphoreType.DMA((10,)),
        ],
        grant=GRANT,
    )


def edges_kernel(keep, got, cols, outer, mid):
    core = core_of()
    for which, out in enumerate((cols, outer, mid)):
        for f in range(2):
            part = slice((2 * which + f) * PART, (2 * which + f + 1) * PART)
            for piece in range(2):
                at = (2 * f + piece) * PART
                out[at : at + PART, :] = jnp.where(core == piece, keep[part, :], got[part, :])


def outputs_kernel(own, own_winds, got, got_wind, mass, east, north, wind, geo, press, fill, sem):
    core = core_of()
    copies = []

    def write(source, out, which):
        rows = pl.ds(pl.multiple_of(which * RX, RX), RX)
        copies.append(pltpu.make_async_copy(source, out.at[:, rows, :], sem.at[len(copies)]))
        copies[-1].start()

    for f, out in enumerate((wind, geo, press)):
        write(own.at[f], out, core)
    write(got_wind.at[pl.ds(1, HALF)], wind, 1 - core)
    for f, out in enumerate((east, north)):
        write(own_winds.at[f], out, core)
        write(got.at[f], out, 1 - core)
    flux = level_flux * mass[...]
    for f, out in enumerate((geo, press)):
        for k in range(HALF):
            if f == 0:
                fill[0, k] = got[2, k] + geo_rate * got_wind[k + 1]
            else:
                fill[1, k] = got[3, k] - flux * (got_wind[k + 2] - got_wind[k])
        write(fill.at[f], out, 1 - core)
    for copy in copies:
        copy.wait()


def write_out(body, count, scratch, *args):
    return call(
        body,
        [shape(HALF, 2 * RX, LN)] * count,
        args,
        out_specs=[HBM] * count,
        scratch=[*scratch, pltpu.SemaphoreType.DMA((2 * count,))],
    )


def inner_kernel(first, *refs):
    if first:
        ins, (got, mass, east_out, north_out, star, ends) = refs[:3], refs[3:]
    else:
        (press, east, north, wind, geo, mass, east_fix) = refs[:7]
        (east_out, north_out, star, ends, heave, geo_out) = refs[7:]
    core = core_of()
    row = lax.broadcasted_iota(jnp.int32, (8, LN), 0)
    zero = jnp.zeros((8, LN), F32)

    def row_difference(tiles):
        above = [pltpu.roll(tile, 7, 0) for tile in tiles] + [zero]
        below = [zero] + [pltpu.roll(tile, 1, 0) for tile in tiles]
        return [
            jnp.where(row == 7, above[t + 1], above[t]) - jnp.where(row == 0, below[t], below[t + 1])
            for t in range(TILES)
        ]

    def group(g, carry):
        piece = g // 3

        def tile_at(f, k, t):
            tile = slice(8 * t, 8 * t + 8)
            if not first:
                return (press, east, north)[f][k, tile, :]
            k = k - HALF * piece
            return jnp.where(core == piece, ins[f][k, rows_at(core * RX + 8 * t), :], got[f, k, tile, :])

        rows = rows_at(8 * g)
        end_rows = []
        if not first:
            e_fix = east_fix[rows, :]
        for j in range(4):
            k = 4 * g + j
            p = [tile_at(PRESS, k, t) for t in range(TILES)]
            end_rows += [p[0][0:1], p[-1][7:8]]
            e = [tile_at(EAST, k, t) for t in range(TILES)]
            if not first:
                e[0] = e[0] + jnp.where(row == 0, e_fix[2 * j : 2 * j + 1], 0.0)
                e[-1] = e[-1] + jnp.where(row == 7, e_fix[2 * j + 1 : 2 * j + 2], 0.0)
            e = [tile - horiz_push * step for tile, step in zip(e, row_difference(p))]
            spread = row_difference(e)
            for t in range(TILES):
                tile = slice(8 * t, 8 * t + 8)
                east_out[k, tile, :] = e[t]
                n = tile_at(NORTH, k, t)
                n = n - horiz_push * (roll_lanes(p[t], -1) - roll_lanes(p[t], 1))
                north_out[k, tile, :] = n
                divergence = spread[t] + (roll_lanes(n, -1) - roll_lanes(n, 1))
                star[k, tile, :] = p[t] - mass_flux * mass[tile, :] * divergence
                if not first:
                    moved = wind[k + 1, tile, :]
                    geo_now = geo[k, tile, :] + geo_rate * moved
                    geo_out[k, tile, :] = geo_now
                    heave[k, tile, :] = moved + buoy_coupling * geo_now
        ends[rows, :] = jnp.concatenate(end_rows, 0)
        return carry

    lax.fori_loop(0, LV // 4, group, 0)


def inner(first, *args):
    field = shape(LV, RX, LN)
    return call(
        functools.partial(inner_kernel, first),
        [field, field, field, shape(EDGE, LN)] + ([] if first else [field, field]),
        args,
    )


def heave_kernel(wind, geo, got, after, heave, geo_out):
    core = core_of()
    rows = pl.ds(pl.multiple_of(core * RX, RX), RX)

    def level(k, carry):
        here, there = core * HALF + k, (1 - core) * HALF + k
        geo_out[here] = geo[k, rows, :]
        heave[here] = wind[k, rows, :] + buoy_coupling * geo[k, rows, :]
        geo_out[there] = got[GEO, k]
        heave[there] = got[WIND, k] + buoy_coupling * got[GEO, k]
        return carry

    lax.fori_loop(0, HALF, level, 0)


def rim_kernel(first, last, *refs):
    (star_in, heave, ends, mass, rate, up, down, mid, outer, across, around, own_cols) = refs[:12]
    refs = refs[12:]
    if not first:
        (north_fix_in, east_edge, north_own, north_edge), refs = refs[:4], refs[4:]
    (star, forced, to_across, to_far, to_around, east_fix, north_fix) = refs[:7]
    if not last:
        east_edge_out, north_own_out, north_edge_out = refs[7:]
    core, chip = core_of(), chip_of()
    lane = lanes()
    quarter = lane % 4
    second = (quarter < 2) == (lax.rem(lax.axis_index("gy"), 2) == 0)
    rim_lane = jnp.logical_or(lane < 2, lane >= LN - 2)
    row = lax.broadcasted_iota(jnp.int32, (8, LN), 0)
    odd = row % 2 == 1
    ratio, inverse, scale = rate[0], rate[1], rate[3]

    for g in range(LV // 4):
        rows = slice(8 * g, 8 * g + 8)
        more = slice(EDGE + 8 * g, EDGE + 8 * g + 8)
        p_low = jnp.where(core == 0, outer[rows, :], mid[rows, :])
        p_high = jnp.where(core == 0, mid[rows, :], outer[rows, :])
        p_edge = jnp.where(second, around[rows, :], across[rows, :])
        p_own = own_cols[rows, :]
        if first:
            e_edge = jnp.where(
                odd,
                jnp.where(core == 0, outer[more, :], mid[more, :]),
                jnp.where(core == 0, mid[more, :], outer[more, :]),
            )
            n_own, n_edge = own_cols[more, :], jnp.where(second, around[more, :], across[more, :])
        else:
            e_edge, n_own, n_edge = east_edge[rows, :], north_own[rows, :], north_edge[rows, :]
        own_up, own_down = roll_lanes(p_own, -1), roll_lanes(p_own, 1)
        edge_up, edge_down = roll_lanes(p_edge, -1), roll_lanes(p_edge, 1)
        low_side = quarter == 1
        n_edge = n_edge - horiz_push * jnp.where(low_side, own_up - edge_down, edge_up - own_down)
        n_own = n_own - horiz_push * jnp.where(low_side, edge_up - own_down, own_up - edge_down)
        n_fix = -horiz_push * jnp.where(low_side, edge_up - own_up, own_down - edge_down)
        if not first:
            n_fix = n_fix + north_fix_in[rows, :]
        gap = n_edge - (n_own - n_fix)
        north_fix[rows, :] = n_fix
        if not last:
            north_own_out[rows, :] = n_own
            north_edge_out[rows, :] = n_edge
        spread = jnp.where(
            quarter == 0,
            roll_lanes(n_fix, -1),
            jnp.where(
                quarter == 1,
                roll_lanes(gap, -1),
                -jnp.where(quarter == 2, roll_lanes(gap, 1), roll_lanes(n_fix, 1)),
            ),
        )
        tips = ends[rows, :]
        edges, fixes = [], []
        for j in range(4):
            a, b = 2 * j, 2 * j + 1
            over = e_edge[a : a + 1] - horiz_push * (p_high[b : b + 1] - tips[b : b + 1])
            under = e_edge[b : b + 1] - horiz_push * (tips[a : a + 1] - p_low[a : a + 1])
            lift, sink = horiz_push * p_low[b : b + 1], -horiz_push * p_high[a : a + 1]
            edges += [over, under]
            fixes += [lift, sink]
            for t in range(TILES):
                tile = slice(8 * t, 8 * t + 8)
                term = jnp.where(rim_lane, roll_lanes(spread, 126 - 4 * (8 * j + t)), 0.0)
                if t == 0:
                    term = term - jnp.where(row == 0, under, jnp.where(row == 1, lift, 0.0))
                if t == TILES - 1:
                    term = term + jnp.where(row == 7, over, jnp.where(row == 6, sink, 0.0))
                k = 4 * g + j
                star[k, tile, :] = star_in[k, tile, :] - mass_flux * mass[tile, :] * term
        if not last:
            east_edge_out[rows, :] = jnp.concatenate(edges, 0)
        east_fix[rows, :] = jnp.concatenate(fixes, 0)

    for t in range(TILES):
        tile = slice(8 * t, 8 * t + 8)
        rho, inv, factor = ratio[tile], inverse[tile], scale[tile]
        bottom, top = factor * star[0, tile, :], factor * star[LV - 1, tile, :]
        total = -up[0, tile, :] * bottom
        tail = -inv * down[0, tile, :] * bottom
        power = None
        for k in range(LV):
            f = heave[k, tile, :]
            if k < LV - 1:
                f = f - star[k + 1, tile, :]
            if k > 0:
                f = f + star[k - 1, tile, :]
            f = factor * f
            forced[k, tile, :] = f
            total = rho * total + up[k + 1, tile, :] * f
            weighted = down[k + 1, tile, :] * f
            tail = tail + (weighted if k == 0 else power * weighted)
            power = rho if k == 0 else power * rho
        total = total + inv * up[LV + 1, tile, :] * top
        tail = tail + power * (down[LV + 1, tile, :] * top)
        even = lax.rem(chip, 2) == 0
        low = chip < 2
        to_across[0, tile, :] = jnp.where(even, total, tail)
        to_across[1, tile, :] = jnp.where(even, top, bottom)
        to_around[0, tile, :] = jnp.where(low, total, tail)
        to_around[1, tile, :] = jnp.where(low, top, bottom)
        to_far[tile, :] = jnp.where(low, total, tail)


def rim(first, last, *args):
    edge, field, pair = shape(EDGE, LN), shape(LV, RX, LN), shape(2, RX, LN)
    return call(
        functools.partial(rim_kernel, first, last),
        [field, field, pair, shape(RX, LN), pair] + [edge] * (2 if last else 5),
        args,
    )


def solve_kernel(last, *refs):
    (star, forced, geo, mass, rate, up, down, from_across, from_far, from_around) = refs[:10]
    refs = refs[10:]
    if last:
        (mine, wind_theirs, sums, wind, geo_out, press) = refs
    else:
        (wind, press, mid, outer, cols, sums) = refs
    core, chip = core_of(), chip_of()

    for t in range(TILES):
        tile = slice(8 * t, 8 * t + 8)
        ratio, inverse, deep, scale = (rate[i, tile, :] for i in range(4))
        zero = jnp.zeros((8, LN), F32)
        near, far, turn = from_across[0, tile, :], deep * from_far[tile, :], from_around[0, tile, :]
        even = lax.rem(chip, 2) == 0
        star_near, star_turn = from_across[1, tile, :], from_around[1, tile, :]
        star_under = jnp.where(even, jnp.where(chip == 2, star_turn, zero), star_near)
        star_over = jnp.where(even, star_near, jnp.where(chip == 1, star_turn, zero))
        turn = jnp.where((chip == 0) | (chip == 3), deep * deep * turn, turn)
        enter = jnp.where(even, zero, near) + jnp.where(chip >= 2, far + turn, zero)
        above = jnp.where(even, near, zero) + jnp.where(chip <= 1, far + turn, zero)
        enter = enter - inverse * up[1, tile, :] * star_under - up[0, tile, :] * (scale * star[0, tile, :])
        above = above + inverse * down[LV, tile, :] * star_over + down[LV + 1, tile, :] * (scale * star[LV - 1, tile, :])

        def force(k):
            f = forced[k, tile, :]
            if k == 0:
                f = f + star_under
            if k == LV - 1:
                f = f - star_over
            return f

        total = enter
        for k in range(LV):
            total = ratio * total + up[k + 1, tile, :] * force(k)
            sums[k, tile, :] = total
        carried = ratio * above
        higher = down[LV + 1, tile, :] * (ratio * total) + up[LV + 1, tile, :] * above
        wind[LV + 1, tile, :] = higher
        flux = level_flux * mass[tile, :]
        here = None
        for k in range(LV - 1, -1, -1):
            solved = down[k + 1, tile, :] * sums[k, tile, :] + up[k + 1, tile, :] * carried
            wind[k + 1, tile, :] = solved
            if last:
                geo_out[k, tile, :] = geo[k, tile, :] + geo_rate * solved
            if k < LV - 1:
                press[k + 1, tile, :] = star[k + 1, tile, :] - flux * (higher - solved)
                higher = here
            here = solved
            carried = ratio * (carried + down[k + 1, tile, :] * force(k))
        lowest = down[0, tile, :] * enter + up[0, tile, :] * carried
        wind[0, tile, :] = lowest
        press[0, tile, :] = star[0, tile, :] - flux * (higher - lowest)

    if last:
        here, there = core * HALF, (1 - core) * HALF
        for k in range(HALF):
            for f, (source, off) in enumerate(((wind, 1), (geo_out, 0), (press, 0))):
                mine[f, k] = source[here + k + off]
        for k in range(HALF + 2):
            wind_theirs[k] = wind[there + k]
    else:
        for g, (first_rows, last_rows) in enumerate(zip(*pack_rows(tiles_of(press), LV // 4))):
            rows = slice(8 * g, 8 * g + 8)
            mid[rows, :] = jnp.where(core == 0, last_rows, first_rows)
            outer[rows, :] = jnp.where(core == 0, first_rows, last_rows)
        pack_columns([(tiles_of(press), 4 * g, cols, 8 * g) for g in range(LV // 4)])


def solve(last, *args):
    edge, field, tall = shape(EDGE, LN), shape(LV, RX, LN), shape(LV + 2, RX, LN)
    if last:
        outs = [shape(3, HALF, RX, LN), shape(HALF + 2, RX, LN)]
        scratch = [pltpu.VMEM(s.shape, F32) for s in (field, tall, field, field)]
    else:
        outs = [tall, field, edge, edge, edge]
        scratch = [pltpu.VMEM(field.shape, F32)]
    return call(functools.partial(solve_kernel, last), outs, args, scratch=scratch)


def sort_kernel(east, north, east_fix, north_fix, geo, star, mine, theirs):
    core = core_of()
    lane = lanes()
    inner_lane = jnp.logical_or(lane == 0, lane == LN - 1)
    row = lax.broadcasted_iota(jnp.int32, (8, LN), 0)

    def group(g, carry):
        for out, piece in ((mine, core), (theirs, 1 - core)):
            rows = rows_at(8 * (3 * piece + g))
            e_fix, n_fix = east_fix[rows, :], north_fix[rows, :]
            for j in range(4):
                k = HALF * piece + 4 * g + j
                for t in range(TILES):
                    tile = slice(8 * t, 8 * t + 8)
                    e, n = east[k, tile, :], north[k, tile, :]
                    if t == 0:
                        e = e + jnp.where(row == 0, e_fix[2 * j : 2 * j + 1], 0.0)
                    if t == TILES - 1:
                        e = e + jnp.where(row == 7, e_fix[2 * j + 1 : 2 * j + 2], 0.0)
                    n = n + jnp.where(inner_lane, roll_lanes(n_fix, 126 - 4 * (8 * j + t)), 0.0)
                    out[0, 4 * g + j, tile, :] = e
                    out[1, 4 * g + j, tile, :] = n
                if out is theirs:
                    out[2, 4 * g + j] = geo[k]
                    out[3, 4 * g + j] = star[k]
        return carry

    lax.fori_loop(0, 3, group, 0)


def local(east_wind, north_wind, vertical_wind, geopotential, pressure, column_mass):
    columns, tiles, pieces = lax.axis_size("gx"), lax.axis_size("gy"), lax.axis_size("gz")
    core, chip = core_of(), chip_of()
    swap = [(i, i ^ 1) for i in range(pieces)]

    across_chip = [(i, i ^ 2) for i in range(pieces)]
    around_chip = [(i, (pieces // 2 - 1 - i // 2) * 2 + i % 2) for i in range(pieces)]
    far_chip = [(i, (i + 4) % pieces) for i in range(pieces)]
    outward = [
        (a * pieces + z, (a + (1 if z % 2 else -1)) % columns * pieces + (z ^ 1))
        for a in range(columns)
        for z in range(pieces)
    ]
    across_tile = [(i, i ^ 1) for i in range(tiles)]
    around_tile = [(i, tiles - 1 - i) for i in range(tiles)]
    if tiles != 4 or pieces != 8:
        raise ValueError("sizes")

    fields = (pressure, east_wind, north_wind, vertical_wind, geopotential)
    send, keep, give = split(*fields)
    got_edges = lax.ppermute(give, "gz", swap)
    wide = shape(2 * EDGE, LN)
    send, got_edges = lax.optimization_barrier((send, got_edges))
    got = lax.ppermute(send, "gz", swap)
    cols, outer, mid = call(edges_kernel, [wide] * 3, [keep, got_edges])

    mass = lax.dynamic_slice_in_dim(column_mass, core * RX, RX, 0)
    stiff_ratio = stiffness * mass
    root = jnp.sqrt(1.0 + 4.0 * stiff_ratio)
    ratio = (1.0 + 2.0 * stiff_ratio - root) / (2.0 * stiff_ratio)
    log_ratio = jnp.log(ratio)
    level = (chip * LV - 1 + lax.iota(jnp.int32, LV + 2)).astype(F32)[:, None, None]
    up = 1.0 - jnp.exp((2.0 * (level + 1.0)) * log_ratio)
    down = 1.0 - jnp.exp((2.0 * (NZ - level)) * log_ratio)
    scale = 1.0 / (root * (1.0 - jnp.exp((2.0 * (NZ + 1.0)) * log_ratio)))
    rate = jnp.stack([ratio, 1.0 / ratio, jnp.exp(float(LV) * log_ratio), scale])

    field = shape(LV, RX, LN)
    for substep in range(ITERS):
        first, last = substep == 0, substep == ITERS - 1
        across = lax.ppermute(cols, "gy", across_tile)
        around = lax.ppermute(cols, "gy", around_tile)
        outer_in = lax.ppermute(outer, ("gx", "gz"), outward)
        if first:
            mid_in = mid
            east, north, star, ends = inner(first, *fields[:3], got, mass)
            heave, geo = call(heave_kernel, [field, field], [*fields[3:], got, ends])
        else:
            mid_in = lax.ppermute(mid, "gz", swap)
            east, north, star, ends, heave, geo = inner(first, press, east, north, wind, geo, mass, east_fix)
        args = [star, heave, ends, mass, rate, up, down, mid_in, outer_in, across, around, cols]
        if not first:
            args += [north_fix, *edges]
        star, forced, to_across, to_far, to_around, east_fix, north_fix, *edges = rim(first, last, *args)
        from_far = lax.ppermute(to_far, "gz", far_chip)
        from_across = lax.ppermute(to_across, "gz", across_chip)
        from_around = lax.ppermute(to_around, "gz", around_chip)
        args = [star, forced, geo, mass, rate, up, down, from_across, from_far, from_around]
        if last:
            own_part, send_part = call(
                sort_kernel,
                [shape(2, HALF, RX, LN), shape(4, HALF, RX, LN)],
                [east, north, east_fix, north_fix, geo, star],
            )
            got_part = lax.ppermute(send_part, "gz", swap)
            solved, send_solved = solve(last, *args)
            got_solved = lax.ppermute(send_solved, "gz", swap)
            other = lax.dynamic_slice_in_dim(column_mass, (1 - core) * RX, RX, 0)
            fill = pltpu.VMEM((2, HALF, RX, LN), F32)
            outputs = write_out(outputs_kernel, 5, (fill,), solved, own_part, got_part, got_solved, other)
        else:
            wind, press, mid, outer, cols = solve(last, *args)
    return tuple(outputs)


def solution(mesh):
    spec = P("gz", "gx", "gy")
    return jax.shard_map(
        local, mesh=mesh, in_specs=(spec,) * 5 + (P("gx", "gy"),), out_specs=(spec,) * 5, check_vma=False
    )
```
